256 devices in a mesh: tp: 32 (over z, y), dp: 8 (over x, core).
Axes of the slice: x: 4, y: 4, z: 8, core: 2. Of those that a mesh axis runs over, the one named last changes fastest.
Arguments:
- hidden_in: bfloat16 [8192, 2048], P('dp')
- targets: bfloat16 [8192, 2048], P('dp')
- w_up: bfloat16 [4, 2048, 8192], P(None, None, 'tp')
- w_down: bfloat16 [4, 8192, 2048], P(None, 'tp')
Outputs:
- output 1: float32 [4, 2048, 8192], P(None, None, 'tp')
- output 2: float32 [4, 8192, 2048], P(None, 'tp')
All inputs are finite; a program needn't handle non-finite values.
Results may differ from the reference program's by a relative error of at most 0.0111594.
Values are sent between devices in bfloat16 or wider.
A program may use at most 768 MiB of HBM per device.

```python
import math
import jax
import jax.numpy as jnp
from jax import lax

D = 2048
FF = 8192
TOKENS = 8192
BLOCK_ROWS = 512
LAYERS = 4


def setup_inputs(seed: int = 0) -> dict:
    keys = jax.random.split(jax.random.key(seed), 4)
    tgt_scale = 2.0 * math.sqrt(TOKENS)
    hidden_in = jax.random.normal(keys[0], (TOKENS, D), jnp.float32)
    targets = tgt_scale * jax.random.normal(keys[1], (TOKENS, D), jnp.float32)
    w_up = jax.random.normal(keys[2], (LAYERS, D, FF), jnp.float32) * (D ** -0.5)
    w_down = jax.random.normal(keys[3], (LAYERS, FF, D), jnp.float32) * (FF ** -0.5)
    return {"hidden_in": hidden_in.astype(jnp.bfloat16), "targets": targets.astype(jnp.bfloat16), "w_up": w_up.astype(jnp.bfloat16), "w_down": w_down.astype(jnp.bfloat16)}


def gelu_tanh(value):
    return jax.nn.gelu(value, approximate=True)


def block_grads(hidden, target, w_up, w_down):
    def fwd_layer(h_cur, weights):
        up_w, down_w = weights
        pre_act = jnp.dot(h_cur, up_w, preferred_element_type=jnp.float32).astype(jnp.bfloat16)
        act_val = gelu_tanh(pre_act.astype(jnp.float32)).astype(jnp.bfloat16)
        branch = jnp.dot(act_val, down_w, preferred_element_type=jnp.float32).astype(jnp.bfloat16)
        return h_cur + branch, (h_cur, pre_act, act_val)

    h_last, saved = lax.scan(fwd_layer, hidden, (w_up, w_down))
    err_f32 = (h_last.astype(jnp.float32) - target.astype(jnp.float32)) / TOKENS

    def bwd_layer(g_cur, layer_in):
        h_in, pre_act, act_val, up_w, down_w = layer_in
        g_down = jnp.dot(act_val.T, g_cur, preferred_element_type=jnp.float32)
        d_act = jnp.dot(g_cur, down_w.T, preferred_element_type=jnp.float32)
        _, gelu_vjp = jax.vjp(gelu_tanh, pre_act.astype(jnp.float32))
        d_pre = gelu_vjp(d_act)[0].astype(jnp.bfloat16)
        g_up = jnp.dot(h_in.T, d_pre, preferred_element_type=jnp.float32)
        back_sum = g_cur.astype(jnp.float32) + jnp.dot(d_pre, up_w.T, preferred_element_type=jnp.float32)
        return back_sum.astype(jnp.bfloat16), (g_up, g_down)

    _, grads = lax.scan(bwd_layer, err_f32.astype(jnp.bfloat16), (saved[0], saved[1], saved[2], w_up, w_down), reverse=True)
    return grads


def reference(hidden_in, targets, w_up, w_down):
    num_blocks = TOKENS // BLOCK_ROWS
    hid_blocks = hidden_in.reshape(num_blocks, BLOCK_ROWS, D)
    tgt_blocks = targets.reshape(num_blocks, BLOCK_ROWS, D)

    def accumulate(acc_grads, block_pair):
        g_up, g_down = block_grads(block_pair[0], block_pair[1], w_up, w_down)
        return (acc_grads[0] + g_up, acc_grads[1] + g_down), None

    zero_grads = (jnp.zeros((LAYERS, D, FF), jnp.float32), jnp.zeros((LAYERS, FF, D), jnp.float32))
    (grad_up, grad_down), _ = lax.scan(accumulate, zero_grads, (hid_blocks, tgt_blocks))
    return grad_up, grad_down
```

```python
import functools
import jax
import jax.numpy as jnp
from jax import lax
from jax.experimental import pallas as pl
from jax.experimental.pallas import tpu as pltpu
from jax.sharding import PartitionSpec as P

NZ = 8
NY = 4
ROW_CONTRACT = (((0,), (0,)), ((), ()))
COL_CONTRACT = (((1,), (1,)), ((), ()))
CHAINS = ((0, 0, 4), (1, 0, 3), (1, 1, 4), (0, 1, 3))
ANY = pl.BlockSpec(memory_space=pl.ANY)
VMEM = pl.BlockSpec(memory_space=pltpu.VMEM)


def gelu_tanh(value):
    return jax.nn.gelu(value, approximate=True)


def place():
    tp = lax.axis_index("tp")
    return lax.div(tp, NY), lax.rem(tp, NY)


def entry_barrier(z, y, with_z):
    peers = [(z, lax.rem(y + s, NY)) for s in (1, 2, 3)]
    if with_z:
        peers += [(lax.rem(z + 1, NZ), y), (lax.rem(z + NZ - 1, NZ), y)]
    sem = pltpu.get_barrier_semaphore()
    for pz, py in peers:
        pl.semaphore_signal(sem, inc=1, device_id={"tp": pz * NY + py}, device_id_type=pl.DeviceIdType.MESH)
    pl.semaphore_wait(sem, len(peers))


def remote(src, dst, send_sem, recv_sem, pz, py):
    return pltpu.make_async_remote_copy(
        src_ref=src, dst_ref=dst, send_sem=send_sem, recv_sem=recv_sem,
        device_id={"tp": pz * NY + py}, device_id_type=pl.DeviceIdType.MESH)


class RowGather:
    def __init__(self, block, out, z, y, local_sem, send_sem, recv_sem):
        rows = block.shape[0]
        half = rows // 2
        up, down = lax.rem(y + 1, NY), lax.rem(y + NY - 1, NY)
        own = out.at[pl.ds(pl.multiple_of(y * rows, rows), rows)]
        lower = out.at[pl.ds(pl.multiple_of(down * rows, rows), half)]
        upper = out.at[pl.ds(pl.multiple_of(up * rows + half, half), half)]
        self.local = pltpu.make_async_copy(block, own, local_sem)
        self.first = [remote(block, own, send_sem.at[0], recv_sem.at[0], z, up),
                      remote(block, own, send_sem.at[1], recv_sem.at[1], z, down)]
        self.second = [remote(lower, lower, send_sem.at[2], recv_sem.at[2], z, up),
                       remote(upper, upper, send_sem.at[3], recv_sem.at[3], z, down)]

    def start(self):
        self.local.start()
        for copy in self.first:
            copy.start()

    def relay(self):
        for copy, onward in zip(self.first, self.second):
            copy.wait_recv()
            onward.start()

    def finish(self):
        self.local.wait()
        for copy in self.first:
            copy.wait_send()
        for copy in self.second:
            copy.wait()


class ColumnExchange:
    def __init__(self, block, out, z, y, local_sem, send_sem, recv_sem):
        rows, cols = block.shape[0], block.shape[1] // NY
        own = out.at[pl.ds(pl.multiple_of(y * rows, rows), rows)]

        def columns(index):
            return block.at[:, pl.ds(pl.multiple_of(index * cols, cols), cols)]

        self.local = pltpu.make_async_copy(columns(y), own, local_sem)
        self.copies = []
        for s in (1, 2, 3):
            dest = lax.rem(y + s, NY)
            self.copies.append(remote(columns(dest), own, send_sem.at[s - 1], recv_sem.at[s - 1], z, dest))

    def start(self):
        self.local.start()
        for copy in self.copies:
            copy.start()

    def finish(self):
        self.local.wait()
        for copy in self.copies:
            copy.wait()


class SumGather:
    def __init__(self, part, slots, out, z, y, send_sem, recv_sem):
        self.part, self.slots, self.out, self.z, self.y = part, slots, out, z, y
        self.send_sem, self.recv_sem = send_sem, recv_sem
        self.rows, self.cols = part.shape[0] // NZ, part.shape[1] // 2
        self.copies = []
        self.last = {}

    def block(self, ref, owner, half):
        return ref.at[pl.ds(pl.multiple_of(owner * self.rows, self.rows), self.rows), pl.ds(half * self.cols, self.cols)]

    def shifted(self, direction, amount):
        return lax.rem(self.z + (amount if direction == 0 else NZ - amount), NZ)

    def send(self, index, src, dst, direction):
        copy = remote(src, dst, self.send_sem.at[index], self.recv_sem.at[index], self.shifted(direction, 1), self.y)
        copy.start()
        self.copies.append(copy)
        return copy

    def reduce_step(self, chain, step):
        direction, half, hops = CHAINS[chain]
        mine = self.block(self.part, self.shifted(direction, hops - step), half)
        if step > 0:
            self.last[chain].wait_recv()
            mine[...] = mine[...] + self.slots[chain * 4 + step - 1]
        index = chain * 4 + step
        self.last[chain] = self.send(index, mine, self.slots.at[index], direction)

    def reduce_rest(self):
        for step in (1, 2, 3):
            for chain, (_, _, hops) in enumerate(CHAINS):
                if step < hops:
                    self.reduce_step(chain, step)

    def total(self, half):
        value = self.block(self.part, self.z, half)[...]
        for chain, (_, h, hops) in enumerate(CHAINS):
            if h == half:
                self.last[chain].wait_recv()
                value = value + self.slots[chain * 4 + hops - 1]
        return value

    def gather_step(self, chain, step):
        direction, half, hops = CHAINS[chain]
        if step > 0:
            self.last[chain].wait_recv()
        held = self.block(self.out, self.shifted(1 - direction, step) if step else self.z, half)
        self.last[chain] = self.send(16 + chain * 4 + step, held, held, direction)

    def gather(self, steps):
        for step in steps:
            for chain, (_, _, hops) in enumerate(CHAINS):
                if step < hops:
                    self.gather_step(chain, step)

    def finish(self):
        for copy in self.last.values():
            copy.wait_recv()
        for copy in self.copies:
            copy.wait_send()


def forward_kernel(is_last, gather_h, total_tokens, *refs):
    refs = list(refs)
    h_ref, wu_hbm, wd_hbm = refs[:3]
    refs = refs[3:]
    t_ref = refs.pop(0) if is_last else None
    out_ref, u_ref, a_out = refs[:3]
    refs = refs[3:]
    h_out = refs.pop(0) if gather_h else None
    wu, wd, act, part, slots, wsem, lsem, ysend, yrecv, zsend, zrecv = refs
    blocks = wd_hbm.shape[0]
    ucols = wu.shape[1] // 4
    dcols = wd.shape[1] // blocks
    z, y = place()

    def wu_copy(n):
        cols = pl.ds(pl.multiple_of(n * ucols, ucols), ucols)
        return pltpu.make_async_copy(wu_hbm.at[:, cols], wu.at[:, cols], wsem.at[n])

    def wd_copy(n):
        cols = pl.ds(pl.multiple_of(n * dcols, dcols), dcols)
        return pltpu.make_async_copy(wd_hbm.at[n], wd.at[:, cols], wsem.at[4 + n])

    for n in range(4):
        wu_copy(n).start()
    for n in range(blocks):
        wd_copy(n).start()
    entry_barrier(z, y, True)
    if gather_h:
        rows = RowGather(h_ref, h_out, z, y, lsem.at[1], ysend.at[pl.ds(3, 4)], yrecv.at[pl.ds(3, 4)])
        rows.start()

    @pl.loop(0, 4)
    def _(n):
        wu_copy(n).wait()
        cols = pl.ds(pl.multiple_of(n * ucols, ucols), ucols)
        pre = jnp.dot(h_ref[...], wu[:, cols], preferred_element_type=jnp.float32).astype(jnp.bfloat16)
        u_ref[:, cols] = pre
        act[:, cols] = gelu_tanh(pre.astype(jnp.float32)).astype(jnp.bfloat16)

    sums = SumGather(part, slots, out_ref, z, y, zsend, zrecv)
    exchange = ColumnExchange(act, a_out, z, y, lsem.at[0], ysend.at[pl.ds(0, 3)], yrecv.at[pl.ds(0, 3)])

    def down(n):
        wd_copy(n).wait()
        cols = pl.ds(pl.multiple_of(n * dcols, dcols), dcols)
        part[:, cols] = jnp.dot(act[...], wd[:, cols], preferred_element_type=jnp.float32)

    pl.loop(0, blocks // 2)(down)
    sums.reduce_step(0, 0)
    sums.reduce_step(1, 0)
    pl.loop(blocks // 2, blocks)(down)
    sums.reduce_step(2, 0)
    sums.reduce_step(3, 0)
    exchange.start()
    sums.reduce_rest()
    for half in (0, 1):
        branch = sums.total(half).astype(jnp.bfloat16)
        value = sums.block(h_ref, z, half)[...] + branch
        if is_last:
            half_cols = pl.ds(half * sums.cols, sums.cols)
            err = value.astype(jnp.float32) - t_ref[:, half_cols].astype(jnp.float32)
            value = (err / total_tokens).astype(jnp.bfloat16)
        sums.block(out_ref, z, half)[...] = value
    sums.gather((0, 1))
    if gather_h:
        rows.relay()
    sums.gather((2, 3))
    sums.finish()
    exchange.finish()
    if gather_h:
        rows.finish()


def backward_kernel(has_sum, *refs):
    refs = list(refs)
    g_ref, wd_hbm, u_ref = refs[:3]
    refs = refs[3:]
    wu_hbm = refs.pop(0) if has_sum else None
    out_ref = refs.pop(0) if has_sum else None
    du_out, g_out = refs[:2]
    refs = refs[2:]
    if has_sum:
        wd, dpre, wsem, lsem, ysend, yrecv, wu, part, slots, zsend, zrecv = refs
    else:
        wd, dpre, wsem, lsem, ysend, yrecv = refs
    blocks = wd_hbm.shape[0]
    dcols = wd.shape[1] // blocks
    urows = wd.shape[0] // 4
    z, y = place()

    def wd_copy(n):
        return pltpu.make_async_copy(wd_hbm.at[n], wd.at[:, pl.ds(n * dcols, dcols)], wsem.at[n])

    for n in range(blocks):
        wd_copy(n).start()
    if has_sum:
        wu_copy = pltpu.make_async_copy(wu_hbm, wu, wsem.at[blocks])
        wu_copy.start()
    entry_barrier(z, y, has_sum)
    rows = RowGather(g_ref, g_out, z, y, lsem.at[1], ysend.at[pl.ds(3, 4)], yrecv.at[pl.ds(3, 4)])
    rows.start()
    for n in range(blocks):
        wd_copy(n).wait()

    @pl.loop(0, 4)
    def _(n):
        at = pl.ds(pl.multiple_of(n * urows, urows), urows)
        d_act = lax.dot_general(g_ref[...], wd[at, :], COL_CONTRACT, preferred_element_type=jnp.float32)
        _, gelu_vjp = jax.vjp(gelu_tanh, u_ref[:, at].astype(jnp.float32))
        dpre[:, at] = gelu_vjp(d_act)[0].astype(jnp.bfloat16)

    exchange = ColumnExchange(dpre, du_out, z, y, lsem.at[0], ysend.at[pl.ds(0, 3)], yrecv.at[pl.ds(0, 3)])
    if not has_sum:
        exchange.start()
        rows.relay()
        exchange.finish()
        rows.finish()
        return
    wu_copy.wait()
    sums = SumGather(part, slots, out_ref, z, y, zsend, zrecv)
    tile = wu.shape[0] // 8

    def back(n):
        at = pl.ds(pl.multiple_of(n * tile, tile), tile)
        part[:, at] = lax.dot_general(dpre[...], wu[at, :], COL_CONTRACT, preferred_element_type=jnp.float32)

    pl.loop(0, 4)(back)
    sums.reduce_step(0, 0)
    sums.reduce_step(1, 0)
    pl.loop(4, 8)(back)
    sums.reduce_step(2, 0)
    sums.reduce_step(3, 0)
    exchange.start()
    sums.reduce_rest()
    for half in (0, 1):
        total = sums.total(half)
        sums.block(out_ref, z, half)[...] = (sums.block(g_ref, z, half)[...].astype(jnp.float32) + total).astype(jnp.bfloat16)
    sums.gather((0, 1))
    rows.relay()
    sums.gather((2, 3))
    sums.finish()
    exchange.finish()
    rows.finish()


def params(collective_id):
    return pltpu.CompilerParams(collective_id=collective_id, has_side_effects=True, vmem_limit_bytes=48 * 1024 * 1024)


def sum_scratch(rows, width):
    return [pltpu.VMEM((rows, width), jnp.float32), pltpu.VMEM((16, rows // NZ, width // 2), jnp.float32)]


SUM_SEMS = [pltpu.SemaphoreType.DMA((32,)), pltpu.SemaphoreType.DMA((32,))]
Y_SEMS = [pltpu.SemaphoreType.DMA((2,)), pltpu.SemaphoreType.DMA((7,)), pltpu.SemaphoreType.DMA((7,))]


def forward_block(h_cur, w_up, w_down, targets, gather_h, total_tokens, collective_id):
    rows, width = h_cur.shape
    hidden = w_up.shape[1]
    outs = [jax.ShapeDtypeStruct((rows, width), jnp.bfloat16), jax.ShapeDtypeStruct((rows, hidden), jnp.bfloat16),
            jax.ShapeDtypeStruct((rows * NY, hidden // NY), jnp.bfloat16)]
    out_specs = [VMEM, VMEM, ANY]
    args, in_specs = [h_cur, w_up, w_down], [VMEM, ANY, ANY]
    if targets is not None:
        args.append(targets)
        in_specs.append(VMEM)
    if gather_h:
        outs.append(jax.ShapeDtypeStruct((rows * NY, width), jnp.bfloat16))
        out_specs.append(ANY)
    part, slots = sum_scratch(rows, width)
    return pl.pallas_call(
        functools.partial(forward_kernel, targets is not None, gather_h, total_tokens),
        out_shape=outs, in_specs=in_specs, out_specs=out_specs,
        scratch_shapes=[pltpu.VMEM((width, hidden), jnp.bfloat16), pltpu.VMEM((hidden, width), jnp.bfloat16),
                        pltpu.VMEM((rows, hidden), jnp.bfloat16), part, slots,
                        pltpu.SemaphoreType.DMA((4 + w_down.shape[0],))] + Y_SEMS + SUM_SEMS,
        compiler_params=params(collective_id), name="fwd",
        cost_estimate=pl.CostEstimate(flops=40_000_000_000, bytes_accessed=20_000_000, transcendentals=0),
    )(*args)


def backward_block(g_cur, w_up, w_down, pre_act, has_sum, collective_id):
    rows, width = g_cur.shape
    hidden = w_up.shape[1]
    outs = [jax.ShapeDtypeStruct((rows * NY, hidden // NY), jnp.bfloat16), jax.ShapeDtypeStruct((rows * NY, width), jnp.bfloat16)]
    out_specs = [ANY, ANY]
    args, in_specs = [g_cur, w_down, pre_act], [VMEM, ANY, VMEM]
    scratch = [pltpu.VMEM((hidden, width), jnp.bfloat16), pltpu.VMEM((rows, hidden), jnp.bfloat16),
               pltpu.SemaphoreType.DMA((w_down.shape[0] + 1,))] + Y_SEMS
    if has_sum:
        outs.insert(0, jax.ShapeDtypeStruct((rows, width), jnp.bfloat16))
        out_specs.insert(0, VMEM)
        args.append(w_up)
        in_specs.append(ANY)
        part, slots = sum_scratch(rows, width)
        scratch += [pltpu.VMEM((width, hidden), jnp.bfloat16), part, slots] + SUM_SEMS
    return pl.pallas_call(
        functools.partial(backward_kernel, has_sum),
        out_shape=outs, in_specs=in_specs, out_specs=out_specs, scratch_shapes=scratch,
        compiler_params=params(collective_id), name="bwd",
        cost_estimate=pl.CostEstimate(flops=40_000_000_000, bytes_accessed=20_000_000, transcendentals=0),
    )(*args)


def gather_weights(up_piece, down_piece):
    groups = [[z * NY + y for y in range(NY)] for z in range(NZ)]
    both = lax.all_gather(jnp.stack([up_piece, down_piece]), "tp", axis_index_groups=groups)
    ny, _, _, cols = both.shape
    up = both[:, 0].transpose(1, 0, 2).reshape(up_piece.shape[0], ny * up_piece.shape[1])
    down = both[:, 1].reshape(ny * down_piece.shape[0], down_piece.shape[1])
    return lax.all_gather(up, "dp", axis=0, tiled=True), lax.all_gather(down, "dp", axis=0)


def local_step(hidden, targets, w_up, w_down, n_dp):
    layers, width, cols = w_up.shape
    tp, dp = lax.axis_index("tp"), lax.axis_index("dp")
    z, y = lax.div(tp, NY), lax.rem(tp, NY)
    rows = hidden.shape[0] // NY
    piece = width // n_dp
    weights = []
    for layer in range(layers):
        up_piece = lax.dynamic_slice(w_up[layer], (dp * piece, 0), (piece, cols))
        down_piece = lax.dynamic_slice(w_down[layer], (0, dp * piece), (cols, piece))
        weights.append(gather_weights(up_piece, down_piece))
    h_cur = lax.dynamic_slice(hidden, (y * rows, 0), (rows, width))
    t_own = lax.dynamic_slice(targets, (y * rows + z * (rows // NZ), 0), (rows // NZ, width))
    saved = []
    h_all = [hidden]
    for layer in range(layers):
        last = layer == layers - 1
        outs = forward_block(h_cur, *weights[layer], t_own if last else None, layer > 0, hidden.shape[0] * n_dp, layer)
        h_cur, pre_act, act_all = outs[:3]
        if layer > 0:
            h_all.append(outs[3])
        saved.append((pre_act, act_all))
    g_cur = h_cur
    grads_up, grads_down = [None] * layers, [None] * layers
    for layer in reversed(range(layers)):
        pre_act, act_all = saved[layer]
        outs = backward_block(g_cur, *weights[layer], pre_act, layer > 0, layers + layer)
        if layer > 0:
            g_cur = outs[0]
        du_all, g_all = outs[-2:]
        g_down = lax.dot_general(act_all, g_all, ROW_CONTRACT, preferred_element_type=jnp.float32)
        g_up = lax.dot_general(h_all[layer], du_all, ROW_CONTRACT, preferred_element_type=jnp.float32)
        if layer < layers - 1:
            g_down, g_up, grads_down[layer + 1], grads_up[layer + 1] = lax.optimization_barrier(
                (g_down, g_up, grads_down[layer + 1], grads_up[layer + 1]))
        grads_down[layer], grads_up[layer] = lax.psum((g_down, g_up), "dp")
    return jnp.stack(grads_up), jnp.stack(grads_down)


def solution(mesh):
    n_dp = mesh.shape["dp"]

    def grad_step(hidden_in, targets, w_up, w_down):
        step_fn = functools.partial(local_step, n_dp=n_dp)
        mapped = jax.shard_map(step_fn, mesh=mesh, in_specs=(P("dp", None), P("dp", None), P(None, None, "tp"), P(None, "tp", None)), out_specs=(P(None, None, "tp"), P(None, "tp", None)), check_vma=False)
        return mapped(hidden_in, targets, w_up, w_down)

    return grad_step
```

```python
import functools
import jax
import jax.numpy as jnp
from jax import lax
from jax.experimental import pallas as pl
from jax.experimental.pallas import tpu as pltpu
from jax.sharding import PartitionSpec as P

NZ, NY, NX = 8, 4, 4
COPIES, LOCALS = 96, 32
ROW_CONTRACT = (((0,), (0,)), ((), ()))
COL_CONTRACT = (((1,), (1,)), ((), ()))
Z_CHAINS = ((0, 0, 4), (1, 0, 3), (1, 1, 4), (0, 1, 3))
X_CHAINS = ((0, 0, 2), (1, 0, 1), (1, 1, 2), (0, 1, 1))
ANY = pl.BlockSpec(memory_space=pl.ANY)
VMEM = pl.BlockSpec(memory_space=pltpu.VMEM)
BF16, F32 = jnp.bfloat16, jnp.float32


def gelu_tanh(value):
    return jax.nn.gelu(value, approximate=True)


def at(start, size):
    return pl.ds(pl.multiple_of(start, size), size)


def shift(position, amount, size):
    return lax.rem(position + amount % size, size)


class Net:
    def __init__(self, send_sem, recv_sem, local_sem):
        tp, dp = lax.axis_index("tp"), lax.axis_index("dp")
        self.z, self.y = lax.div(tp, NY), lax.rem(tp, NY)
        self.x, self.c = lax.div(dp, 2), lax.rem(dp, 2)
        self.send_sem, self.recv_sem, self.local_sem = send_sem, recv_sem, local_sem
        self.n_copies = self.n_locals = 0

    def device(self, dz=0, dy=0, dx=0, other_core=False):
        z, y, x = shift(self.z, dz, NZ), shift(self.y, dy, NY), shift(self.x, dx, NX)
        c = 1 - self.c if other_core else self.c
        return {"tp": z * NY + y, "dp": x * 2 + c}

    def barrier(self, **axes):
        peers = []
        if axes.get("y"):
            peers += [self.device(dy=s) for s in (1, 2, 3)]
        if axes.get("z"):
            peers += [self.device(dz=s) for s in (1, -1)]
        if axes.get("x"):
            peers += [self.device(dx=s) for s in (1, -1)] + [self.device(other_core=True)]
        sem = pltpu.get_barrier_semaphore()
        for peer in peers:
            pl.semaphore_signal(sem, inc=1, device_id=peer, device_id_type=pl.DeviceIdType.MESH)
        pl.semaphore_wait(sem, len(peers))

    def copy(self, src, dst, **where):
        index = self.n_copies
        self.n_copies += 1
        return pltpu.make_async_remote_copy(
            src_ref=src, dst_ref=dst, send_sem=self.send_sem.at[index], recv_sem=self.recv_sem.at[index],
            device_id=self.device(**where), device_id_type=pl.DeviceIdType.MESH)

    def local(self, src, dst):
        index = self.n_locals
        self.n_locals += 1
        return pltpu.make_async_copy(src, dst, self.local_sem.at[index])


class RowGather:
    def __init__(self, net, block, out):
        rows = block.shape[0]
        half = rows // 2
        below, above = shift(net.y, -1, NY), shift(net.y, 1, NY)
        own = out.at[at(net.y * rows, rows)]
        lower, upper = out.at[at(below * rows, half)], out.at[at(above * rows + half, half)]
        self.local = net.local(block, own)
        self.first = [net.copy(block, own, dy=1), net.copy(block, own, dy=-1)]
        self.second = [net.copy(lower, lower, dy=1), net.copy(upper, upper, dy=-1)]

    def start(self):
        self.local.start()
        for copy in self.first:
            copy.start()

    def relay(self):
        for copy, onward in zip(self.first, self.second):
            copy.wait_recv()
            onward.start()

    def finish(self):
        self.local.wait()
        for copy in self.first:
            copy.wait_send()
        for copy in self.second:
            copy.wait()


class ColumnExchange:
    def __init__(self, net, block, out):
        rows, cols = block.shape[0], block.shape[1] // NY
        own = out.at[at(net.y * rows, rows)]
        self.local = net.local(block.at[:, 0:cols], own)
        self.copies = [net.copy(block.at[:, s * cols:(s + 1) * cols], own, dy=s) for s in (1, 3, 2)]

    def start(self):
        self.local.start()
        for copy in self.copies:
            copy.start()

    def finish(self):
        self.local.wait()
        for copy in self.copies:
            copy.wait()


class PieceFetch:
    def __init__(self, net, w_up, w_down, up, down):
        piece = up.shape[1]
        cols = w_down.shape[0]
        dp = net.x * 2 + net.c
        up_piece, down_piece = w_up.at[at(dp * piece, piece)], w_down.at[:, at(dp * piece, piece)]
        self.copies = []
        for s in (1, 3, 2):
            slot = NY - s - 1
            self.copies.append(net.copy(up_piece, up.at[slot], dy=s))
            self.copies.append(net.copy(down_piece, down.at[slot * cols:(slot + 1) * cols], dy=s))

    def start(self):
        for copy in self.copies:
            copy.start()

    def finish(self):
        for copy in self.copies:
            copy.wait()


class PieceSpread:
    def __init__(self, net, up, down, all_up, all_down):
        piece, tall = up.shape[1], down.shape[0]

        def views(dx, half=None):
            dp = shift(net.x, dx, NX) * 2 + net.c
            if half is None:
                return all_up.at[:, at(dp * piece, piece)], all_down.at[dp]
            return (all_up.at[:, at(dp * piece + half * (piece // 2), piece // 2)],
                    all_down.at[dp, half * (tall // 2):(half + 1) * (tall // 2)])

        own = views(0)
        self.local = [net.local(a, b) for a, b in zip((up, down), own)]
        self.first = [[net.copy(a, b, dx=d) for a, b in zip((up, down), own)] for d in (1, -1)]
        self.second = [[net.copy(v, v, dx=d) for v in views(-d, half)] for half, d in ((0, 1), (1, -1))]
        self.across = [[net.copy(a, b, other_core=True) for a, b in zip((up, down), own)]]
        self.across += [[net.copy(v, v, other_core=True) for v in views(d)] for d in (-1, 1, 2)]

    def start(self):
        for copies in (self.local, *self.first, self.across[0]):
            for copy in copies:
                copy.start()

    def relay(self):
        for first, second, across in zip(self.first, self.second, self.across[1:3]):
            for copy in first:
                copy.wait_recv()
            for copy in (*second, *across):
                copy.start()

    def cross(self):
        for copies in self.second:
            for copy in copies:
                copy.wait_recv()
        for copy in self.across[3]:
            copy.start()

    def finish(self):
        for copy in self.local:
            copy.wait()
        for copies in (*self.first, *self.second):
            for copy in copies:
                copy.wait_send()
        for copies in self.across:
            for copy in copies:
                copy.wait()


class Ring:
    def __init__(self, net, axis, chains, part, slot, out):
        self.net, self.axis, self.chains = net, axis, chains
        self.size = {"x": NX, "z": NZ}[axis]
        self.here = {"x": net.x, "z": net.z}[axis]
        self.part, self.slot, self.out = part, slot, out
        self.copies, self.last = [], {}

    def owner(self, direction, amount):
        return shift(self.here, amount if direction == 0 else -amount, self.size)

    def send(self, chain, src, dst):
        direction = self.chains[chain][0]
        copy = self.net.copy(src, dst, **{"d" + self.axis: 1 if direction == 0 else -1})
        copy.start()
        self.copies.append(copy)
        self.last[chain] = copy

    def reduce(self, chain, step):
        direction, half, hops = self.chains[chain]
        if step >= hops:
            return
        mine = self.part(self.owner(direction, hops - step), half)
        if step > 0:
            self.last[chain].wait_recv()
            mine[...] = mine[...] + self.slot(chain, step - 1)[...]
        self.send(chain, mine, self.slot(chain, step))

    def reduce_half(self, half):
        for chain, (_, h, _) in enumerate(self.chains):
            if h == half:
                self.reduce(chain, 0)

    def reduce_all(self, step):
        for chain in range(len(self.chains)):
            self.reduce(chain, step)

    def total(self, half):
        value = self.part(self.here, half)[...]
        for chain, (_, h, hops) in enumerate(self.chains):
            if h == half:
                self.last[chain].wait_recv()
                value = value + self.slot(chain, hops - 1)[...]
        return value

    def gather(self, chain, step, first=None):
        direction, half, hops = self.chains[chain]
        if step >= hops:
            return
        if step > 0:
            self.last[chain].wait_recv()
        held = self.out(self.owner(direction, -step), half)
        self.send(chain, held if first is None else first, held)

    def gather_all(self, step):
        for chain in range(len(self.chains)):
            self.gather(chain, step)

    def arrived(self):
        for copy in self.last.values():
            copy.wait_recv()

    def finish(self):
        for copy in self.copies:
            copy.wait_send()


def slot_index(chains, chain, step):
    return sum(hops for _, _, hops in chains[:chain]) + step


def z_ring(net, part, slots, out):
    rows, cols = part.shape[0] // NZ, part.shape[1] // 2

    def block(ref):
        return lambda owner, half: ref.at[at(owner * rows, rows), half * cols:(half + 1) * cols]

    ring = Ring(net, "z", Z_CHAINS, block(part), lambda chain, step: slots.at[slot_index(Z_CHAINS, chain, step)], block(out))
    ring.block = block
    return ring


class GradSum:
    def __init__(self, net, act, g_all, h_all, d_pre, out_up, out_down, scratch):
        (self.act, self.g, self.h, self.d, self.up, self.down, self.sib_up, self.sib_down, slots_up, slots_down) = scratch
        self.net, self.outs = net, (out_up, out_down)
        self.loads = [net.local(a, b) for a, b in zip((act, g_all, h_all, d_pre), (self.act, self.g, self.h, self.d))]
        parts, slots = (self.up, self.down), (slots_up, slots_down)

        def slot(chain, step):
            half = X_CHAINS[chain][1]
            before = sum(hops for _, h, hops in X_CHAINS[:chain] if h == half)
            return slots[half].at[before + step]

        self.ring = Ring(net, "x", X_CHAINS, lambda owner, half: parts[half].at[owner, net.c], slot,
                         lambda owner, half: self.outs[half].at[owner, net.c])
        other = 1 - net.c
        self.swap = [net.copy(self.up.at[:, other], self.sib_up, other_core=True),
                     net.copy(self.down.at[:, other], self.sib_down, other_core=True)]
        self.across, self.local = [], []

    def load(self):
        for copy in self.loads:
            copy.start()

    def products(self):
        for copy in self.loads:
            copy.wait()
        tall, wide = self.up.shape[2], self.up.shape[3]
        rows = self.down.shape[2]

        @pl.loop(0, 2 * NX)
        def _(n):
            cols = at(n * tall, tall)
            self.up[lax.div(n, 2), lax.rem(n, 2)] = lax.dot_general(self.h[:, cols], self.d[...], ROW_CONTRACT, preferred_element_type=F32)

        self.swap[0].start()

        @pl.loop(0, 2 * NX)
        def _(n):
            cols = at(n * tall, tall)
            tile = lax.dot_general(self.act[...], self.g[:, cols], ROW_CONTRACT, preferred_element_type=F32)
            self.down[:, :, :, cols] = tile.reshape(NX, 2, rows, tall)

        self.swap[1].start()

    def merge(self):
        c = self.net.c
        for half, (mine, other) in enumerate(((self.up, self.sib_up), (self.down, self.sib_down))):
            self.swap[half].wait_recv()
            for k in range(NX):
                mine[k, c] = mine[k, c] + other[k]
            self.ring.reduce_half(half)

    def cross(self, src, dst):
        copy = self.net.copy(src, dst, other_core=True)
        copy.start()
        self.across.append(copy)

    def settle(self):
        x, c = self.net.x, self.net.c
        for half, mine in enumerate((self.up, self.down)):
            own = mine.at[x, c]
            own[...] = self.ring.total(half)
            out = self.outs[half].at[x, c]
            for chain, (_, h, _) in enumerate(X_CHAINS):
                if h == half:
                    self.ring.gather(chain, 0, own)
            copy = self.net.local(own, out)
            copy.start()
            self.local.append(copy)
            self.cross(own, out)

    def finish(self):
        self.ring.gather_all(1)
        for half in (0, 1):
            for dx in (1, -1):
                out = self.outs[half].at[shift(self.net.x, dx, NX), self.net.c]
                if (half == 0) != (dx == 1):
                    self.cross(out, out)
        self.ring.arrived()
        for half in (0, 1):
            for dx in (1, -1):
                out = self.outs[half].at[shift(self.net.x, dx, NX), self.net.c]
                if (half == 0) == (dx == 1):
                    self.cross(out, out)
            out = self.outs[half].at[shift(self.net.x, 2, NX), self.net.c]
            self.cross(out, out)
        for copy in self.local:
            copy.wait()
        for copy in self.swap:
            copy.wait_send()
        self.ring.finish()
        for copy in self.across:
            copy.wait()


class Weights:
    def __init__(self, net, w_up, w_down, all_up, all_down, wu, wd):
        cols, blocks = w_down.shape[0], all_down.shape[0]
        piece = all_down.shape[2]
        self.up = []
        if wu is not None:
            self.up = [net.local(w_up, wu.at[:, 0:cols])]
            self.up += [net.local(all_up.at[s], wu.at[:, (s + 1) * cols:(s + 2) * cols]) for s in range(NY - 1)]
        self.down = [net.local(w_down, wd.at[0:cols])]
        self.down += [net.local(all_down.at[n], wd.at[cols:, n * piece:(n + 1) * piece]) for n in range(blocks)]

    def start(self, copies):
        for copy in copies:
            copy.start()

    def wait(self, copies):
        for copy in copies:
            copy.wait()


def take(refs, count):
    taken = refs[:count]
    del refs[:count]
    return taken if count > 1 else taken[0]


def start_kernel(*refs):
    refs = list(refs)
    w_up, w_down, all_up, all_down, next_up, next_down, up, down = take(refs, 8)
    net = Net(*refs)
    net.barrier(y=True, x=True)
    fetch = PieceFetch(net, w_up.at[0], w_down.at[0], up, down)
    ahead = PieceFetch(net, w_up.at[1], w_down.at[1], next_up, next_down)
    spread = PieceSpread(net, up, down, all_up, all_down)
    fetch.start()
    fetch.finish()
    spread.start()
    ahead.start()
    spread.relay()
    spread.cross()
    spread.finish()
    ahead.finish()


def forward_kernel(layer, layers, total_tokens, *refs):
    refs = list(refs)
    is_last, gather_h, spreads, fetches = layer == layers - 1, layer > 0, layer + 1 < layers, layer + 2 < layers
    h_ref, w_up, w_down, all_up, all_down = take(refs, 5)
    t_ref = take(refs, 1) if is_last else None
    held = take(refs, 2) if spreads else None
    out_ref, u_ref, a_out = take(refs, 3)
    h_out = take(refs, 1) if gather_h else None
    nexts = take(refs, 2) if spreads else None
    fetched = take(refs, 2) if fetches else None
    wu, wd, act, part, slots = take(refs, 5)
    net = Net(*refs)
    weights = Weights(net, w_up.at[layer], w_down.at[layer], all_up, all_down, wu, wd)
    weights.start(weights.up)
    weights.start(weights.down)
    net.barrier(y=True, z=True, x=spreads)
    if gather_h:
        rows = RowGather(net, h_ref, h_out)
        rows.start()
    if spreads:
        spread = PieceSpread(net, *held, *nexts)
        spread.start()
    if fetches:
        fetch = PieceFetch(net, w_up.at[layer + 2], w_down.at[layer + 2], *fetched)
    cols = wu.shape[1] // NY
    weights.wait(weights.up)

    @pl.loop(0, NY)
    def _(n):
        block = at(n * cols, cols)
        pre = jnp.dot(h_ref[...], wu[:, block], preferred_element_type=F32).astype(BF16)
        u_ref[:, block] = pre
        act[:, block] = gelu_tanh(pre.astype(F32)).astype(BF16)

    ring = z_ring(net, part, slots, out_ref)
    exchange = ColumnExchange(net, act, a_out)
    tile = part.shape[1] // 8

    def down(n):
        part[:, at(n * tile, tile)] = jnp.dot(act[...], wd[:, at(n * tile, tile)], preferred_element_type=F32)

    weights.wait(weights.down)
    pl.loop(0, 4)(down)
    ring.reduce_half(0)
    pl.loop(4, 8)(down)
    ring.reduce_half(1)
    exchange.start()
    if fetches:
        fetch.start()
    for step in (1, 2, 3):
        ring.reduce_all(step)
    for half in (0, 1):
        branch = ring.total(half).astype(BF16)
        value = ring.block(h_ref)(net.z, half)[...] + branch
        if is_last:
            width = value.shape[1]
            err = value.astype(F32) - t_ref[:, half * width:(half + 1) * width].astype(F32)
            value = (err / total_tokens).astype(BF16)
        ring.out(net.z, half)[...] = value
    ring.gather_all(0)
    if spreads:
        spread.relay()
    ring.gather_all(1)
    if gather_h:
        rows.relay()
    ring.gather_all(2)
    ring.gather_all(3)
    if spreads:
        spread.cross()
    ring.arrived()
    ring.finish()
    exchange.finish()
    if fetches:
        fetch.finish()
    if gather_h:
        rows.finish()
    if spreads:
        spread.finish()


def backward_kernel(layer, layers, *refs):
    refs = list(refs)
    has_sum, has_grads = layer > 0, layer < layers - 1
    g_ref, u_ref, w_up, w_down, all_up, all_down = take(refs, 6)
    terms = take(refs, 4) if has_grads else None
    du_out, g_out = take(refs, 2)
    out_ref = take(refs, 1) if has_sum else None
    sums = take(refs, 2) if has_grads else None
    wd, dpre = take(refs, 2)
    if has_sum:
        wu, part, slots = take(refs, 3)
    scratch = take(refs, 10) if has_grads else None
    net = Net(*refs)
    weights = Weights(net, w_up.at[layer], w_down.at[layer], all_up, all_down, wu if has_sum else None, wd)
    weights.start(weights.down)
    if has_sum:
        weights.start(weights.up)
    if has_grads:
        grads = GradSum(net, *terms, *sums, scratch)
        grads.load()
    net.barrier(y=True, z=has_sum, x=has_grads)
    rows = RowGather(net, g_ref, g_out)
    rows.start()
    weights.wait(weights.down)
    cols = wd.shape[0] // NY

    @pl.loop(0, NY)
    def _(n):
        block = at(n * cols, cols)
        d_act = lax.dot_general(g_ref[...], wd[block, :], COL_CONTRACT, preferred_element_type=F32)
        _, gelu_vjp = jax.vjp(gelu_tanh, u_ref[:, block].astype(F32))
        dpre[:, block] = gelu_vjp(d_act)[0].astype(BF16)

    exchange = ColumnExchange(net, dpre, du_out)
    if not has_sum:
        exchange.start()
        grads.products()
        grads.merge()
        grads.ring.reduce_all(1)
        rows.relay()
        grads.settle()
        exchange.finish()
        rows.finish()
        grads.finish()
        return
    weights.wait(weights.up)
    ring = z_ring(net, part, slots, out_ref)
    tile = wu.shape[0] // 8

    def back(n):
        part[:, at(n * tile, tile)] = lax.dot_general(dpre[...], wu[at(n * tile, tile), :], COL_CONTRACT, preferred_element_type=F32)

    pl.loop(0, 4)(back)
    ring.reduce_half(0)
    pl.loop(4, 8)(back)
    ring.reduce_half(1)
    exchange.start()
    if has_grads:
        grads.products()
    ring.reduce_all(1)
    if has_grads:
        grads.merge()
    ring.reduce_all(2)
    ring.reduce_all(3)
    for half in (0, 1):
        total = ring.total(half)
        ring.out(net.z, half)[...] = (ring.block(g_ref)(net.z, half)[...].astype(F32) + total).astype(BF16)
    ring.gather_all(0)
    if has_grads:
        grads.ring.reduce_all(1)
    ring.gather_all(1)
    rows.relay()
    ring.gather_all(2)
    if has_grads:
        grads.settle()
    ring.gather_all(3)
    ring.arrived()
    ring.finish()
    exchange.finish()
    rows.finish()
    if has_grads:
        grads.finish()


def last_kernel(*refs):
    refs = list(refs)
    terms, sums, scratch = take(refs, 4), take(refs, 2), take(refs, 10)
    net = Net(*refs)
    grads = GradSum(net, *terms, *sums, scratch)
    grads.load()
    net.barrier(x=True)
    grads.products()
    grads.merge()
    grads.ring.reduce_all(1)
    grads.settle()
    grads.finish()


def call(kernel, name, collective_id, args, in_specs, outs, out_specs, scratch):
    sems = [pltpu.SemaphoreType.DMA((COPIES,)), pltpu.SemaphoreType.DMA((COPIES,)), pltpu.SemaphoreType.DMA((LOCALS,))]
    return pl.pallas_call(
        kernel, out_shape=outs, in_specs=in_specs, out_specs=out_specs, scratch_shapes=scratch + sems, name=name,
        compiler_params=pltpu.CompilerParams(collective_id=collective_id, has_side_effects=True, vmem_limit_bytes=60 * 1024 * 1024),
        cost_estimate=pl.CostEstimate(flops=40_000_000_000, bytes_accessed=20_000_000, transcendentals=0),
    )(*args)


class Plan:
    def __init__(self, hidden, w_up, n_dp):
        self.layers, self.width, self.cols = w_up.shape
        self.tokens = hidden.shape[0]
        self.rows = self.tokens // NY
        self.hidden = self.cols * NY
        self.n_dp = n_dp
        self.piece = self.width // n_dp

    def gathered(self):
        return [jax.ShapeDtypeStruct((NY - 1, self.width, self.cols), BF16),
                jax.ShapeDtypeStruct((self.n_dp, (NY - 1) * self.cols, self.piece), BF16)]

    def fetched(self):
        return [jax.ShapeDtypeStruct((NY - 1, self.piece, self.cols), BF16),
                jax.ShapeDtypeStruct(((NY - 1) * self.cols, self.piece), BF16)]

    def sum_scratch(self):
        return [pltpu.VMEM((self.rows, self.width), F32), pltpu.VMEM((14, self.rows // NZ, self.width // 2), F32)]

    def grad_outs(self):
        return [jax.ShapeDtypeStruct((NX, 2, self.width // 8, self.cols), F32),
                jax.ShapeDtypeStruct((NX, 2, self.cols // 8, self.width), F32)]

    def grad_scratch(self):
        up, down = self.grad_outs()
        shapes = [up.shape, down.shape, (NX, *up.shape[2:]), (NX, *down.shape[2:]), (3, *up.shape[2:]), (3, *down.shape[2:])]
        loads = [(self.tokens, self.cols), (self.tokens, self.width), (self.tokens, self.width), (self.tokens, self.cols)]
        return [pltpu.VMEM(s, BF16) for s in loads] + [pltpu.VMEM(s, F32) for s in shapes]


def struct(*shape):
    return jax.ShapeDtypeStruct(shape, BF16)


def vmem(array):
    return pltpu.VMEM(array.shape, array.dtype)


def local_step(hidden, targets, w_up, w_down, n_dp):
    plan = Plan(hidden, w_up, n_dp)
    layers, width, rows = plan.layers, plan.width, plan.rows
    tp = lax.axis_index("tp")
    z, y = lax.div(tp, NY), lax.rem(tp, NY)
    h_cur = lax.dynamic_slice(hidden, (y * rows, 0), (rows, width))
    t_own = lax.dynamic_slice(targets, (y * rows + z * (rows // NZ), 0), (rows // NZ, width))
    outs = call(start_kernel, "start", 0, [w_up, w_down], [ANY, ANY], plan.gathered() + plan.fetched(), [ANY, ANY, VMEM, VMEM],
                [vmem(a) for a in plan.fetched()])
    weights, held = [outs[:2]], outs[2:]
    wu, wd = pltpu.VMEM((width, plan.hidden), BF16), pltpu.VMEM((plan.hidden, width), BF16)
    act = pltpu.VMEM((rows, plan.hidden), BF16)
    saved, h_all = [], [hidden]
    for layer in range(layers):
        args, in_specs = [h_cur, w_up, w_down, *weights[layer]], [VMEM] + [ANY] * 4
        shapes = [struct(rows, width), struct(rows, plan.hidden), struct(plan.tokens, plan.cols)]
        out_specs = [VMEM, VMEM, ANY]
        if layer == layers - 1:
            args.append(t_own)
            in_specs.append(VMEM)
        if layer + 1 < layers:
            args += held
            in_specs += [VMEM, VMEM]
        if layer > 0:
            shapes.append(struct(plan.tokens, width))
            out_specs.append(ANY)
        if layer + 1 < layers:
            shapes += plan.gathered()
            out_specs += [ANY, ANY]
        if layer + 2 < layers:
            shapes += plan.fetched()
            out_specs += [VMEM, VMEM]
        outs = list(call(functools.partial(forward_kernel, layer, layers, plan.tokens * n_dp), "fwd", 1 + layer, args, in_specs,
                         shapes, out_specs, [wu, wd, act] + plan.sum_scratch()))
        h_cur, pre_act, act_all = take(outs, 3)
        saved.append((pre_act, act_all))
        if layer > 0:
            h_all.append(take(outs, 1))
        if layer + 1 < layers:
            weights.append(take(outs, 2))
        held = outs
    g_cur = h_cur
    grads = [None] * layers
    terms = None
    for layer in reversed(range(layers)):
        pre_act, act_all = saved[layer]
        args, in_specs = [g_cur, pre_act, w_up, w_down, *weights[layer]], [VMEM, VMEM] + [ANY] * 4
        shapes, out_specs = [struct(plan.tokens, plan.cols), struct(plan.tokens, width)], [ANY, ANY]
        scratch = [wd, act]
        if layer > 0:
            shapes.append(struct(rows, width))
            out_specs.append(VMEM)
            scratch += [wu] + plan.sum_scratch()
        if terms is not None:
            args += terms
            in_specs += [ANY] * 4
            shapes += plan.grad_outs()
            out_specs += [ANY, ANY]
            scratch += plan.grad_scratch()
        outs = list(call(functools.partial(backward_kernel, layer, layers), "bwd", 1 + layers + layer, args, in_specs, shapes,
                         out_specs, scratch))
        du_all, g_all = take(outs, 2)
        if layer > 0:
            g_cur = take(outs, 1)
        if terms is not None:
            grads[layer + 1] = take(outs, 2)
        terms = [act_all, g_all, h_all[layer], du_all]
    grads[0] = call(last_kernel, "last", 1 + 2 * layers, terms, [ANY] * 4, plan.grad_outs(), [ANY, ANY], plan.grad_scratch())
    up = jnp.stack([g[0].reshape(width, plan.cols) for g in grads])
    down = jnp.stack([g[1].reshape(plan.cols, width) for g in grads])
    return up, down


def solution(mesh):
    n_dp = mesh.shape["dp"]

    def grad_step(hidden_in, targets, w_up, w_down):
        step_fn = functools.partial(local_step, n_dp=n_dp)
        mapped = jax.shard_map(step_fn, mesh=mesh, in_specs=(P("dp", None), P("dp", None), P(None, None, "tp"), P(None, "tp", None)), out_specs=(P(None, None, "tp"), P(None, "tp", None)), check_vma=False)
        return mapped(hidden_in, targets, w_up, w_down)

    return grad_step
```

```python
import functools
import jax
import jax.numpy as jnp
from jax import lax
from jax.experimental import pallas as pl
from jax.experimental.pallas import tpu as pltpu
from jax.sharding import PartitionSpec as P

NZ, NY, NX = 8, 4, 4
COPIES, LOCALS = 512, 160
ROW_CONTRACT = (((0,), (0,)), ((), ()))
COL_CONTRACT = (((1,), (1,)), ((), ()))
Z_CHAINS = ((0, 0, 4), (1, 0, 3), (1, 1, 4), (0, 1, 3))
X_CHAINS = ((0, 0, 2), (1, 0, 1), (1, 1, 2), (0, 1, 1))
ANY = pl.BlockSpec(memory_space=pl.ANY)
VMEM = pl.BlockSpec(memory_space=pltpu.VMEM)
BF16, F32 = jnp.bfloat16, jnp.float32


def gelu_tanh(value):
    return jax.nn.gelu(value, approximate=True)


def at(start, size):
    return pl.ds(pl.multiple_of(start, size), size)


def shift(position, amount, size):
    return lax.rem(position + amount % size, size)


class Net:
    def __init__(self, send_sem, recv_sem, local_sem):
        tp, dp = lax.axis_index("tp"), lax.axis_index("dp")
        self.z, self.y = lax.div(tp, NY), lax.rem(tp, NY)
        self.x, self.c = lax.div(dp, 2), lax.rem(dp, 2)
        self.send_sem, self.recv_sem, self.local_sem = send_sem, recv_sem, local_sem
        self.n_copies = self.n_locals = 0

    def device(self, dz=0, dy=0, dx=0, other_core=False):
        z, y, x = shift(self.z, dz, NZ), shift(self.y, dy, NY), shift(self.x, dx, NX)
        c = 1 - self.c if other_core else self.c
        return {"tp": z * NY + y, "dp": x * 2 + c}

    def barrier(self):
        peers = [self.device(dy=s) for s in (1, 2, 3)] + [self.device(dz=s) for s in (1, -1)]
        peers += [self.device(dx=s) for s in (1, -1)] + [self.device(other_core=True)]
        sem = pltpu.get_barrier_semaphore()
        for peer in peers:
            pl.semaphore_signal(sem, inc=1, device_id=peer, device_id_type=pl.DeviceIdType.MESH)
        pl.semaphore_wait(sem, len(peers))

    def copy(self, src, dst, **where):
        index = self.n_copies
        self.n_copies += 1
        return pltpu.make_async_remote_copy(
            src_ref=src, dst_ref=dst, send_sem=self.send_sem.at[index], recv_sem=self.recv_sem.at[index],
            device_id=self.device(**where), device_id_type=pl.DeviceIdType.MESH)

    def local(self, src, dst):
        index = self.n_locals
        self.n_locals += 1
        return pltpu.make_async_copy(src, dst, self.local_sem.at[index])


class RowGather:
    def __init__(self, net, block, out):
        rows = block.shape[0]
        half = rows // 2
        below, above = shift(net.y, -1, NY), shift(net.y, 1, NY)
        own = out.at[at(net.y * rows, rows)]
        lower, upper = out.at[at(below * rows, half)], out.at[at(above * rows + half, half)]
        self.local = net.local(block, own)
        self.first = [net.copy(block, own, dy=1), net.copy(block, own, dy=-1)]
        self.second = [net.copy(lower, lower, dy=1), net.copy(upper, upper, dy=-1)]

    def start(self):
        self.local.start()
        for copy in self.first:
            copy.start()

    def relay(self):
        for copy, onward in zip(self.first, self.second):
            copy.wait_recv()
            onward.start()

    def sent(self):
        self.local.wait()
        for copy in self.first:
            copy.wait_send()

    def finish(self):
        for copy in self.second:
            copy.wait()


class ColumnExchange:
    def __init__(self, net, block, out):
        rows, cols = block.shape[0], block.shape[1] // NY
        own = out.at[at(net.y * rows, rows)]
        self.local = net.local(block.at[:, 0:cols], own)
        self.copies = [net.copy(block.at[:, s * cols:(s + 1) * cols], own, dy=s) for s in (1, 3, 2)]

    def start(self):
        self.local.start()
        for copy in self.copies:
            copy.start()

    def finish(self):
        self.local.wait()
        for copy in self.copies:
            copy.wait()


class PieceFetch:
    def __init__(self, net, piece, slot):
        self.copies = [net.copy(piece, slot(NY - s - 1), dy=s) for s in (1, 3, 2)]

    def start(self):
        for copy in self.copies:
            copy.start()

    def arrived(self):
        for copy in self.copies:
            copy.wait_recv()

    def sent(self):
        for copy in self.copies:
            copy.wait_send()


class PieceSpread:
    def __init__(self, net, held, view):
        own = view(0, None)
        self.local = net.local(held, own)
        self.first = [net.copy(held, own, dx=d) for d in (1, -1)]
        self.second = [net.copy(view(-d, half), view(-d, half), dx=d) for half, d in ((0, 1), (1, -1))]
        self.across = [net.copy(held, own, other_core=True)]
        self.across += [net.copy(view(d, None), view(d, None), other_core=True) for d in (-1, 1, 2)]

    def start(self):
        for copy in (self.local, *self.first, self.across[0]):
            copy.start()

    def relay(self):
        for first, second, across in zip(self.first, self.second, self.across[1:3]):
            first.wait_recv()
            second.start()
            across.start()

    def cross(self):
        for copy in self.second:
            copy.wait_recv()
        self.across[3].start()

    def finish(self):
        self.local.wait()
        for copy in (*self.first, *self.second):
            copy.wait_send()
        for copy in self.across:
            copy.wait()


class Ring:
    def __init__(self, net, axis, chains, part, slot, out):
        self.net, self.axis, self.chains = net, axis, chains
        self.size = {"x": NX, "z": NZ}[axis]
        self.here = {"x": net.x, "z": net.z}[axis]
        self.part, self.slot, self.out = part, slot, out
        self.copies, self.last = [], {}

    def owner(self, direction, amount):
        return shift(self.here, amount if direction == 0 else -amount, self.size)

    def send(self, chain, src, dst):
        direction = self.chains[chain][0]
        copy = self.net.copy(src, dst, **{"d" + self.axis: 1 if direction == 0 else -1})
        copy.start()
        self.copies.append(copy)
        self.last[chain] = copy

    def reduce(self, chain, step):
        direction, half, hops = self.chains[chain]
        if step >= hops:
            return
        mine = self.part(self.owner(direction, hops - step), half)
        if step > 0:
            self.last[chain].wait_recv()
            mine[...] = mine[...] + self.slot(chain, step - 1)[...]
        self.send(chain, mine, self.slot(chain, step))

    def reduce_half(self, half):
        for chain, (_, h, _) in enumerate(self.chains):
            if h == half:
                self.reduce(chain, 0)

    def reduce_all(self, step):
        for chain in range(len(self.chains)):
            self.reduce(chain, step)

    def total(self, half):
        value = self.part(self.here, half)[...]
        for chain, (_, h, hops) in enumerate(self.chains):
            if h == half:
                self.last[chain].wait_recv()
                value = value + self.slot(chain, hops - 1)[...]
        return value

    def gather(self, chain, step, first=None):
        direction, half, hops = self.chains[chain]
        if step >= hops:
            return
        if step > 0:
            self.last[chain].wait_recv()
        held = self.out(self.owner(direction, -step), half)
        self.send(chain, held if first is None else first, held)

    def gather_half(self, half):
        for chain, (_, h, _) in enumerate(self.chains):
            if h == half:
                self.gather(chain, 0)

    def gather_all(self, step):
        for chain in range(len(self.chains)):
            self.gather(chain, step)

    def arrived(self):
        for copy in self.last.values():
            copy.wait_recv()

    def finish(self):
        for copy in self.copies:
            copy.wait_send()


def slot_index(chains, chain, step):
    return sum(hops for _, _, hops in chains[:chain]) + step


def z_ring(net, part, slots, out):
    rows, cols = part.shape[0] // NZ, part.shape[1] // 2

    def block(ref):
        return lambda owner, half: ref.at[at(owner * rows, rows), half * cols:(half + 1) * cols]

    ring = Ring(net, "z", Z_CHAINS, block(part), lambda chain, step: slots.at[slot_index(Z_CHAINS, chain, step)], block(out))
    ring.block = block
    return ring


class GradSum:
    def __init__(self, net, part, sib, slots, out):
        self.net, self.mine, self.sib, self.out = net, part, sib, out
        half_rows = part.shape[2] // 2

        def block(ref):
            return lambda owner, half: ref.at[owner, net.c, half * half_rows:(half + 1) * half_rows]

        self.ring = Ring(net, "x", X_CHAINS, block(part), lambda chain, step: slots.at[slot_index(X_CHAINS, chain, step)], block(out))
        self.swap = net.copy(part.at[:, 1 - net.c], sib, other_core=True)
        self.across, self.local = [], []

    def merge(self):
        c = self.net.c
        self.swap.wait_recv()
        for k in range(NX):
            self.mine[k, c] = self.mine[k, c] + self.sib[k]
        for half in (0, 1):
            self.ring.reduce_half(half)

    def step(self):
        self.ring.reduce_all(1)

    def cross(self, src, dst):
        copy = self.net.copy(src, dst, other_core=True)
        copy.start()
        self.across.append(copy)

    def settle(self):
        for half in (0, 1):
            own = self.ring.part(self.net.x, half)
            own[...] = self.ring.total(half)
            for chain, (_, h, _) in enumerate(X_CHAINS):
                if h == half:
                    self.ring.gather(chain, 0, own)
        x, c = self.net.x, self.net.c
        self.local = self.net.local(self.mine.at[x, c], self.out.at[x, c])
        self.local.start()
        self.cross(self.mine.at[x, c], self.out.at[x, c])

    def relay(self):
        self.ring.gather_all(1)

    def finish(self):
        self.ring.arrived()
        for dx in (1, -1, 2):
            held = self.out.at[shift(self.net.x, dx, NX), self.net.c]
            self.cross(held, held)
        self.local.wait()
        self.swap.wait_send()
        self.ring.finish()

    def end(self):
        for copy in self.across:
            copy.wait()


def take(refs, count):
    taken = refs[:count]
    del refs[:count]
    return taken if count > 1 else taken[0]


def step_kernel(layers, total_tokens, *refs):
    refs = list(refs)
    h0_ref, t_ref, w_up, w_down, x_all = take(refs, 5)
    grad_up, grad_down = take(refs, 2)
    all_up, all_down, h_all, a_all, g_all, du_all = take(refs, 6)
    wu, wd, rows_buf, u_buf, act, dpre, part, slots = take(refs, 8)
    held_up, held_down = take(refs, 2)
    up_part, up_sib, up_slots, down_part, down_sib, down_slots = take(refs, 6)
    a_in, g_in, h_in, du_in = take(refs, 4)
    net = Net(*refs)
    top = layers - 1
    width, hidden = wu.shape[1], wu.shape[2]
    cols = hidden // NY
    piece = held_up.shape[2]
    tile = width // 8
    dp = net.x * 2 + net.c

    def start(copies):
        for copy in copies:
            copy.start()

    def wait(copies):
        for copy in copies:
            copy.wait()

    def fetch_of(layer):
        return (PieceFetch(net, w_up.at[layer, at(dp * piece, piece)], lambda slot: held_up.at[layer, slot]),
                PieceFetch(net, w_down.at[layer, :, at(dp * piece, piece)], lambda slot: held_down.at[layer, slot * cols:(slot + 1) * cols]))

    def spread_of(layer):
        def up_view(dx, half):
            first = (shift(net.x, dx, NX) * 2 + net.c) * piece
            if half is None:
                return all_up.at[layer, :, at(first, piece)]
            return all_up.at[layer, :, at(first + half * (piece // 2), piece // 2)]

        def down_view(dx, half):
            index, tall = shift(net.x, dx, NX) * 2 + net.c, 3 * cols
            if half is None:
                return all_down.at[layer, index]
            return all_down.at[layer, index, half * (tall // 2):(half + 1) * (tall // 2)]

        return PieceSpread(net, held_up.at[layer], up_view), PieceSpread(net, held_down.at[layer], down_view)

    def up_loads(layer):
        b = layer % 2
        own = net.local(w_up.at[layer], wu.at[b, :, 0:cols])
        return own, [net.local(all_up.at[layer, s], wu.at[b, :, (s + 1) * cols:(s + 2) * cols]) for s in range(NY - 1)]

    def down_loads(layer):
        b = layer % 2
        own = net.local(w_down.at[layer], wd.at[b, 0:cols])
        return own, [net.local(all_down.at[layer, n], wd.at[b, cols:, n * piece:(n + 1) * piece]) for n in range(all_down.shape[1])]

    net.barrier()
    fetches = [fetch_of(0)]
    start(fetches[0])
    fetches.append(fetch_of(1))
    start(fetches[1])
    loads = up_loads(0), down_loads(0)
    loads[0][0].start()
    loads[1][0].start()
    first = net.local(h0_ref, rows_buf.at[0])
    first.start()
    spread_up, spread_down = spread_of(0)
    fetches[0][0].arrived()
    spread_up.start()
    fetches[0][1].arrived()
    spread_down.start()
    spread_up.relay()
    spread_down.relay()
    spread_up.cross()
    spread_up.finish()
    start(loads[0][1])
    first.wait()

    rows = None
    for layer in range(layers):
        b = layer % 2
        h_ref, out_ref = rows_buf.at[b], rows_buf.at[1 - b]
        spreads = None
        if layer > 0:
            rows = RowGather(net, h_ref, h_all.at[layer - 1])
            rows.start()
            if layer < top:
                fetches[layer + 1][0].arrived()
                fetches[layer + 1][1].arrived()
                spreads = spread_of(layer + 1)
                start(spreads)
        loads[0][0].wait()
        wait(loads[0][1])

        @pl.loop(0, NY)
        def _(n):
            block = at(n * cols, cols)
            pre = jnp.dot(h_ref[...], wu[b, :, block], preferred_element_type=F32).astype(BF16)
            u_buf[layer, :, block] = pre
            act[:, block] = gelu_tanh(pre.astype(F32)).astype(BF16)

        exchange = ColumnExchange(net, act, a_all.at[layer])
        if layer == 0:
            exchange.start()
            spread_down.cross()
            spread_down.finish()
            start(loads[1][1])
            fetches[1][0].arrived()
            fetches[1][1].arrived()
            spreads = spread_of(1)
            start(spreads)
        ring = z_ring(net, part, slots, out_ref)

        def down(n):
            part[:, at(n * tile, tile)] = jnp.dot(act[...], wd[b, :, at(n * tile, tile)], preferred_element_type=F32)

        loads[1][0].wait()
        wait(loads[1][1])
        pl.loop(0, 4)(down)
        ring.reduce_half(0)
        pl.loop(4, 8)(down)
        ring.reduce_half(1)
        if layer == 0:
            for ahead in range(2, layers):
                fetches.append(fetch_of(ahead))
                start(fetches[ahead])
        else:
            exchange.start()
        for step in (1, 2, 3):
            ring.reduce_all(step)
        for half in (0, 1):
            value = ring.block(h_ref)(net.z, half)[...] + ring.total(half).astype(BF16)
            if layer == top:
                wide = value.shape[1]
                err = value.astype(F32) - t_ref[:, half * wide:(half + 1) * wide].astype(F32)
                value = (err / total_tokens).astype(BF16)
            ring.out(net.z, half)[...] = value
            ring.gather_half(half)
        if spreads:
            spreads[0].relay()
            spreads[1].relay()
        ring.gather_all(1)
        if layer > 0:
            rows.relay()
        ring.gather_all(2)
        if spreads:
            spreads[0].cross()
            spreads[1].cross()
        ring.gather_all(3)
        if spreads:
            spreads[0].finish()
            spreads[1].finish()
            loads = up_loads(layer + 1), down_loads(layer + 1)
            for own, others in loads:
                own.start()
                start(others)
        if layer > 0:
            rows.sent()
        exchange.finish()
        ring.arrived()
        ring.finish()
        if layer > 0:
            rows.finish()
    for pair in fetches:
        pair[0].sent()
        pair[1].sent()

    def up_product():
        tall = up_part.shape[2]

        @pl.loop(0, 2 * NX)
        def _(n):
            up_part[lax.div(n, 2), lax.rem(n, 2)] = lax.dot_general(
                h_in[:, at(n * tall, tall)], du_in[...], ROW_CONTRACT, preferred_element_type=F32)

    def down_product():
        @pl.loop(0, 8)
        def _(n):
            block = at(n * tile, tile)
            value = lax.dot_general(a_in[...], g_in[:, block], ROW_CONTRACT, preferred_element_type=F32)
            down_part[:, :, :, block] = value.reshape(NX, 2, cols // 8, tile)

    def up_sum_of(layer):
        return GradSum(net, up_part, up_sib, up_slots, grad_up.at[layer])

    def down_sum_of(layer):
        return GradSum(net, down_part, down_sib, down_slots, grad_down.at[layer])

    reload, last_rows, last_up = {}, None, None
    for layer in reversed(range(layers)):
        b = layer % 2
        g_ref, out_ref = rows_buf.at[1 - b], rows_buf.at[b]
        h_load = net.local(x_all if layer == 0 else h_all.at[layer - 1], h_in)
        a_load = net.local(a_all.at[layer], a_in)
        if layer in reload:
            reload[layer][0][0].wait()
            wait(reload[layer][0][1])

        @pl.loop(0, NY)
        def _(n):
            block = at(n * cols, cols)
            d_act = lax.dot_general(g_ref[...], wd[b, block, :], COL_CONTRACT, preferred_element_type=F32)
            _, gelu_vjp = jax.vjp(gelu_tanh, u_buf[layer, :, block].astype(F32))
            dpre[:, block] = gelu_vjp(d_act)[0].astype(BF16)

        exchange = ColumnExchange(net, dpre, du_all.at[layer])
        rows = RowGather(net, g_ref, g_all.at[layer])
        ring = None
        if layer == 0:
            exchange.start()
            rows.start()
        else:
            if layer in reload:
                reload[layer][1][0].wait()
                wait(reload[layer][1][1])
            ring = z_ring(net, part, slots, out_ref)

            def back(n):
                part[:, at(n * tile, tile)] = lax.dot_general(
                    dpre[...], wu[b, at(n * tile, tile), :], COL_CONTRACT, preferred_element_type=F32)

            pl.loop(0, 4)(back)
            ring.reduce_half(0)
            exchange.start()
            rows.start()
            pl.loop(4, 8)(back)
            ring.reduce_half(1)
        down_sum = None
        if last_rows is not None:
            last_rows.finish()
            g_load = net.local(g_all.at[layer + 1], g_in)
            g_load.start()
            last_up.relay()
        if layer >= 2:
            reload[layer - 2] = (down_loads(layer - 2), up_loads(layer - 2)) if layer > 2 else (down_loads(0),)
            for own, others in reload[layer - 2]:
                own.start()
                start(others)
        if last_rows is not None:
            g_load.wait()
            last_a.wait()
            down_sum = down_sum_of(layer + 1)
            down_product()
            down_sum.swap.start()
        a_load.start()
        h_load.start()
        if ring:
            ring.reduce_all(1)
        if down_sum:
            last_up.finish()
            down_sum.merge()
        if ring:
            ring.reduce_all(2)
        if down_sum:
            last_up.end()
        exchange.finish()
        du_load = net.local(du_all.at[layer], du_in)
        du_load.start()
        h_load.wait()
        du_load.wait()
        up_sum = up_sum_of(layer)
        up_product()
        up_sum.swap.start()
        if ring:
            ring.reduce_all(3)
        if down_sum:
            down_sum.step()
        if ring:
            for half in (0, 1):
                total = ring.total(half)
                ring.out(net.z, half)[...] = (ring.block(g_ref)(net.z, half)[...].astype(F32) + total).astype(BF16)
                ring.gather_half(half)
        up_sum.merge()
        if ring:
            ring.gather_all(1)
        rows.relay()
        if down_sum:
            down_sum.settle()
        if ring:
            ring.gather_all(2)
        up_sum.step()
        if ring:
            ring.gather_all(3)
        rows.sent()
        if down_sum:
            down_sum.relay()
        if ring:
            ring.arrived()
            ring.finish()
        if layer > 0:
            up_sum.settle()
        if down_sum:
            down_sum.finish()
            down_sum.end()
        last_rows, last_up, last_a = rows, up_sum, a_load
    last_up.settle()
    last_rows.finish()
    g_load = net.local(g_all.at[0], g_in)
    g_load.start()
    last_up.relay()
    g_load.wait()
    last_a.wait()
    down_sum = down_sum_of(0)
    down_product()
    down_sum.swap.start()
    last_up.finish()
    down_sum.merge()
    down_sum.step()
    down_sum.settle()
    down_sum.relay()
    last_up.end()
    down_sum.finish()
    down_sum.end()


def local_step(hidden, targets, w_up, w_down, n_dp):
    layers, width, cols = w_up.shape
    tokens = hidden.shape[0]
    rows, inner, piece = tokens // NY, cols * NY, width // n_dp
    tp = lax.axis_index("tp")
    z, y = lax.div(tp, NY), lax.rem(tp, NY)
    h_own = lax.dynamic_slice(hidden, (y * rows, 0), (rows, width))
    t_own = lax.dynamic_slice(targets, (y * rows + z * (rows // NZ), 0), (rows // NZ, width))
    up_shape, down_shape = (NX, 2, width // 8, cols), (NX, 2, cols // 8, width)

    def out(dtype, *shape):
        return jax.ShapeDtypeStruct(shape, dtype)

    outs = [out(F32, layers, *up_shape), out(F32, layers, *down_shape),
            out(BF16, layers, NY - 1, width, cols), out(BF16, layers, n_dp, (NY - 1) * cols, piece),
            out(BF16, layers - 1, tokens, width), out(BF16, layers, tokens, cols),
            out(BF16, layers, tokens, width), out(BF16, layers, tokens, cols)]

    def sum_scratch(shape):
        return [pltpu.VMEM(shape, F32), pltpu.VMEM((NX, *shape[2:]), F32), pltpu.VMEM((6, shape[2] // 2, shape[3]), F32)]

    scratch = [pltpu.VMEM((2, width, inner), BF16), pltpu.VMEM((2, inner, width), BF16), pltpu.VMEM((2, rows, width), BF16),
               pltpu.VMEM((layers, rows, inner), BF16), pltpu.VMEM((rows, inner), BF16), pltpu.VMEM((rows, inner), BF16),
               pltpu.VMEM((rows, width), F32), pltpu.VMEM((14, rows // NZ, width // 2), F32),
               pltpu.VMEM((layers, NY - 1, piece, cols), BF16), pltpu.VMEM((layers, (NY - 1) * cols, piece), BF16),
               *sum_scratch(up_shape), *sum_scratch(down_shape),
               pltpu.VMEM((tokens, cols), BF16), pltpu.VMEM((tokens, width), BF16), pltpu.VMEM((tokens, width), BF16), pltpu.VMEM((tokens, cols), BF16),
               pltpu.SemaphoreType.DMA((COPIES,)), pltpu.SemaphoreType.DMA((COPIES,)), pltpu.SemaphoreType.DMA((LOCALS,))]
    up, down = pl.pallas_call(
        functools.partial(step_kernel, layers, tokens * n_dp), out_shape=outs, in_specs=[ANY, VMEM, ANY, ANY, ANY],
        out_specs=[ANY] * len(outs), scratch_shapes=scratch, name="step",
        compiler_params=pltpu.CompilerParams(collective_id=0, has_side_effects=True, vmem_limit_bytes=60 * 1024 * 1024),
    )(h_own, t_own, w_up, w_down, hidden)[:2]
    return up.reshape(layers, width, cols), down.reshape(layers, cols, width)


def solution(mesh):
    n_dp = mesh.shape["dp"]

    def grad_step(hidden_in, targets, w_up, w_down):
        step_fn = functools.partial(local_step, n_dp=n_dp)
        mapped = jax.shard_map(step_fn, mesh=mesh, in_specs=(P("dp", None), P("dp", None), P(None, None, "tp"), P(None, "tp", None)), out_specs=(P(None, None, "tp"), P(None, "tp", None)), check_vma=False)
        return mapped(hidden_in, targets, w_up, w_down)

    return grad_step
```

```python
import functools
import jax
import jax.numpy as jnp
from jax import lax
from jax.experimental import pallas as pl
from jax.experimental.pallas import tpu as pltpu
from jax.sharding import PartitionSpec as P

NZ, NY, NX = 8, 4, 4
COPIES, LOCALS = 832, 160
PARTS = 4
ROW_CONTRACT = (((0,), (0,)), ((), ()))
COL_CONTRACT = (((1,), (1,)), ((), ()))
Z_CHAINS = tuple(chain for q in range(PARTS) for chain in ((q % 2, q, 4), (1 - q % 2, q, 3)))
X_CHAINS = ((0, 0, 2), (1, 0, 1), (1, 1, 2), (0, 1, 1))
ANY = pl.BlockSpec(memory_space=pl.ANY)
BF16, F32 = jnp.bfloat16, jnp.float32


def gelu_tanh(value):
    return jax.nn.gelu(value, approximate=True)


def at(start, size):
    return pl.ds(pl.multiple_of(start, size), size)


class Net:
    def __init__(self, send_sem, recv_sem, local_sem):
        tp, dp = lax.axis_index("tp"), lax.axis_index("dp")
        self.z, self.y = lax.div(tp, NY), lax.rem(tp, NY)
        self.x, self.c = lax.div(dp, 2), lax.rem(dp, 2)
        self.other = 1 - self.c
        self.send_sem, self.recv_sem, self.local_sem = send_sem, recv_sem, local_sem
        self.n_copies = self.n_locals = 0
        self.known = {}

    def near(self, axis, amount):
        size = {"x": NX, "y": NY, "z": NZ}[axis]
        key = axis, amount % size
        if key not in self.known:
            here = getattr(self, axis)
            self.known[key] = lax.rem(here + key[1], size) if key[1] else here
        return self.known[key]

    def span(self, axis, amount, rows):
        key = axis, amount % {"x": NX, "y": NY, "z": NZ}[axis], rows
        if key not in self.known:
            self.known[key] = at(self.near(axis, amount) * rows, rows)
        return self.known[key]

    def block(self, dx):
        key = "block", dx % NX
        if key not in self.known:
            self.known[key] = self.near("x", dx) * 2 + self.c
        return self.known[key]

    def device(self, dz=0, dy=0, dx=0, other_core=False):
        key = "device", dz % NZ, dy % NY, dx % NX, other_core
        if key not in self.known:
            c = self.other if other_core else self.c
            self.known[key] = {"tp": self.near("z", dz) * NY + self.near("y", dy), "dp": self.near("x", dx) * 2 + c}
        return self.known[key]

    def barrier(self):
        peers = [self.device(dy=s) for s in (1, 2, 3)] + [self.device(dz=s) for s in (1, -1)]
        peers += [self.device(dx=s) for s in (1, -1)] + [self.device(other_core=True)]
        sem = pltpu.get_barrier_semaphore()
        for peer in peers:
            pl.semaphore_signal(sem, inc=1, device_id=peer, device_id_type=pl.DeviceIdType.MESH)
        pl.semaphore_wait(sem, len(peers))

    def copy(self, src, dst, **where):
        index = self.n_copies
        self.n_copies += 1
        return pltpu.make_async_remote_copy(
            src_ref=src, dst_ref=dst, send_sem=self.send_sem.at[index], recv_sem=self.recv_sem.at[index],
            device_id=self.device(**where), device_id_type=pl.DeviceIdType.MESH)

    def local(self, src, dst):
        index = self.n_locals
        self.n_locals += 1
        return pltpu.make_async_copy(src, dst, self.local_sem.at[index])


class RowGather:
    def __init__(self, net, block, out):
        rows = block.shape[0]
        half = rows // 2
        own = out.at[net.span("y", 0, rows)]
        lower, upper = out.at[net.span("y", -1, rows)].at[0:half], out.at[net.span("y", 1, rows)].at[half:rows]
        self.local = net.local(block, own)
        self.first = [net.copy(block, own, dy=1), net.copy(block, own, dy=-1)]
        self.second = [net.copy(lower, lower, dy=1), net.copy(upper, upper, dy=-1)]

    def start(self):
        self.local.start()
        for copy in self.first:
            copy.start()

    def relay(self):
        for copy, onward in zip(self.first, self.second):
            copy.wait_recv()
            onward.start()

    def sent(self):
        self.local.wait()
        for copy in self.first:
            copy.wait_send()

    def finish(self):
        for copy in self.second:
            copy.wait()


class ColumnExchange:
    def __init__(self, net, block, out):
        rows, cols = block.shape[0], block.shape[1] // NY
        own = out.at[net.span("y", 0, rows)]
        self.local = net.local(block.at[:, 0:cols], own)
        self.copies = [net.copy(block.at[:, s * cols:(s + 1) * cols], own, dy=s) for s in (1, 3, 2)]

    def start(self):
        self.local.start()
        for copy in self.copies:
            copy.start()

    def sent(self):
        self.local.wait()
        for copy in self.copies:
            copy.wait_send()

    def arrived(self):
        for copy in self.copies:
            copy.wait_recv()


class PieceFetch:
    def __init__(self, net, piece, slot):
        self.copies = [net.copy(piece, slot(NY - s - 1), dy=s) for s in (1, 3, 2)]

    def start(self):
        for copy in self.copies:
            copy.start()

    def arrived(self):
        for copy in self.copies:
            copy.wait_recv()

    def sent(self):
        for copy in self.copies:
            copy.wait_send()


class PieceSpread:
    def __init__(self, net, held, view):
        own = view(0, None)
        self.local = net.local(held, own)
        self.first = [net.copy(held, own, dx=d) for d in (1, -1)]
        self.second = [net.copy(view(-d, half), view(-d, half), dx=d) for half, d in ((0, 1), (1, -1))]
        self.across = [net.copy(held, own, other_core=True)]
        self.across += [net.copy(view(d, None), view(d, None), other_core=True) for d in (-1, 1, 2)]

    def start(self):
        for copy in (self.local, *self.first, self.across[0]):
            copy.start()

    def relay(self):
        for first, second, across in zip(self.first, self.second, self.across[1:3]):
            first.wait_recv()
            second.start()
            across.start()

    def cross(self):
        for copy in self.second:
            copy.wait_recv()
        self.across[3].start()

    def finish(self):
        self.local.wait()
        for copy in (*self.first, *self.second):
            copy.wait_send()
        for copy in self.across:
            copy.wait()


class Ring:
    def __init__(self, net, axis, chains, part, slot, out):
        self.net, self.axis, self.chains = net, axis, chains
        self.part, self.slot, self.out = part, slot, out
        self.copies, self.last = [], {}

    def owner(self, direction, amount):
        return amount if direction == 0 else -amount

    def send(self, chain, src, dst):
        direction = self.chains[chain][0]
        copy = self.net.copy(src, dst, **{"d" + self.axis: 1 if direction == 0 else -1})
        copy.start()
        self.copies.append(copy)
        self.last[chain] = copy

    def reduce(self, chain, step):
        direction, half, hops = self.chains[chain]
        if step >= hops:
            return
        mine = self.part(self.owner(direction, hops - step), half)
        if step > 0:
            self.last[chain].wait_recv()
            mine[...] = mine[...] + self.slot(chain, step - 1)[...]
        self.send(chain, mine, self.slot(chain, step))

    def reduce_half(self, half):
        for chain, (_, h, _) in enumerate(self.chains):
            if h == half:
                self.reduce(chain, 0)

    def reduce_all(self, step, jobs=()):
        self.events(self.reduce, step, jobs)

    def events(self, action, step, jobs):
        jobs = list(jobs)
        for chain, (_, _, hops) in enumerate(self.chains):
            if step < hops:
                action(chain, step)
                if jobs:
                    jobs.pop(0)()
        for job in jobs:
            job()

    def total(self, half):
        value = self.part(0, half)[...]
        for chain, (_, h, hops) in enumerate(self.chains):
            if h == half:
                self.last[chain].wait_recv()
                value = value + self.slot(chain, hops - 1)[...]
        return value

    def gather(self, chain, step, first=None):
        direction, half, hops = self.chains[chain]
        if step >= hops:
            return
        if step > 0:
            self.last[chain].wait_recv()
        held = self.out(self.owner(direction, -step), half)
        self.send(chain, held if first is None else first, held)

    def gather_half(self, half):
        for chain, (_, h, _) in enumerate(self.chains):
            if h == half:
                self.gather(chain, 0)

    def gather_all(self, step, jobs=()):
        self.events(self.gather, step, jobs)

    def arrived(self):
        for copy in self.last.values():
            copy.wait_recv()

    def finish(self):
        for copy in self.copies:
            copy.wait_send()


def slot_index(chains, chain, step):
    return sum(hops for _, _, hops in chains[:chain]) + step


def z_ring(net, part, slots, out):
    rows, cols = part.shape[0] // NZ, part.shape[1] // PARTS

    def block(ref):
        return lambda owner, half: ref.at[net.span("z", owner, rows), half * cols:(half + 1) * cols]

    ring = Ring(net, "z", Z_CHAINS, block(part), lambda chain, step: slots.at[slot_index(Z_CHAINS, chain, step)], block(out))
    ring.block = block
    return ring


class GradSum:
    def __init__(self, net, part, sib, slots, out):
        self.net, self.mine, self.sib, self.out = net, part, sib, out
        half_rows = part.shape[2] // 2

        def block(ref):
            return lambda owner, half: ref.at[net.near("x", owner), net.c, half * half_rows:(half + 1) * half_rows]

        self.ring = Ring(net, "x", X_CHAINS, block(part), lambda chain, step: slots.at[slot_index(X_CHAINS, chain, step)], block(out))
        self.swap = net.copy(part.at[:, net.other], sib, other_core=True)
        self.across, self.local = [], []

    def merge(self):
        c = self.net.c
        self.swap.wait_recv()
        for k in range(NX):
            self.mine[k, c] = self.mine[k, c] + self.sib[k]
        for half in (0, 1):
            self.ring.reduce_half(half)

    def step(self):
        self.ring.reduce_all(1)

    def cross(self, src, dst):
        copy = self.net.copy(src, dst, other_core=True)
        copy.start()
        self.across.append(copy)

    def settle(self):
        for half in (0, 1):
            own = self.ring.part(0, half)
            own[...] = self.ring.total(half)
            for chain, (_, h, _) in enumerate(X_CHAINS):
                if h == half:
                    self.ring.gather(chain, 0, own)
        x, c = self.net.x, self.net.c
        self.local = self.net.local(self.mine.at[x, c], self.out.at[x, c])
        self.local.start()
        self.cross(self.mine.at[x, c], self.out.at[x, c])

    def relay(self):
        self.ring.gather_all(1)

    def finish(self):
        self.ring.arrived()
        for dx in (1, -1, 2):
            held = self.out.at[self.net.near("x", dx), self.net.c]
            self.cross(held, held)
        self.local.wait()
        self.swap.wait_send()
        self.ring.finish()

    def end(self):
        for copy in self.across:
            copy.wait()


def take(refs, count):
    taken = refs[:count]
    del refs[:count]
    return taken if count > 1 else taken[0]


def step_kernel(layers, total_tokens, *refs):
    refs = list(refs)
    x_all, t_all, w_up, w_down = take(refs, 4)
    grad_up, grad_down = take(refs, 2)
    all_up, all_down, h_all, a_all, g_all, du_all = take(refs, 6)
    wu, wd, rows_buf, u_buf, act, dpre, part, slots = take(refs, 8)
    held_up, held_down = take(refs, 2)
    up_part, up_sib, up_slots, down_part, down_sib, down_slots = take(refs, 6)
    a_in, g_in, h_in, du_in, g_last, t_buf = take(refs, 6)
    net = Net(*refs)
    top = layers - 1
    width, hidden = wu.shape[1], wu.shape[2]
    cols = hidden // NY
    piece = held_up.shape[2]
    tile = width // 8
    pieces_at = {dx: at(net.block(dx) * piece, piece) for dx in range(NX)}

    def start(copies):
        for copy in copies:
            copy.start()

    def wait(copies):
        for copy in copies:
            copy.wait()

    own_piece = pieces_at[0]

    def fetch_of(layer):
        return (PieceFetch(net, w_up.at[layer, own_piece], lambda slot: held_up.at[layer, slot]),
                PieceFetch(net, w_down.at[layer, :, own_piece], lambda slot: held_down.at[layer, slot * cols:(slot + 1) * cols]))

    def spread_of(layer):
        def up_view(dx, half):
            whole = all_up.at[layer, :, pieces_at[dx % NX]]
            return whole if half is None else whole.at[:, half * (piece // 2):(half + 1) * (piece // 2)]

        def down_view(dx, half):
            index, tall = net.block(dx), 3 * cols
            if half is None:
                return all_down.at[layer, index]
            return all_down.at[layer, index, half * (tall // 2):(half + 1) * (tall // 2)]

        return PieceSpread(net, held_up.at[layer], up_view), PieceSpread(net, held_down.at[layer], down_view)

    def up_loads(layer):
        b = layer % 2
        own = net.local(w_up.at[layer], wu.at[b, :, 0:cols])
        return own, [net.local(all_up.at[layer, s], wu.at[b, :, (s + 1) * cols:(s + 2) * cols]) for s in range(NY - 1)]

    def down_loads(layer):
        b = layer % 2
        own = net.local(w_down.at[layer], wd.at[b, 0:cols])
        return own, [net.local(all_down.at[layer, n], wd.at[b, cols:, n * piece:(n + 1) * piece]) for n in range(all_down.shape[1])]

    net.barrier()
    fetches = [fetch_of(0)]
    start(fetches[0])
    fetches.append(fetch_of(1))
    start(fetches[1])
    loads = up_loads(0), down_loads(0)
    loads[0][0].start()
    loads[1][0].start()
    n_rows = rows_buf.shape[1]
    n_slice = n_rows // NZ
    first = [net.local(x_all.at[at(net.y * n_rows, n_rows)], rows_buf.at[0]),
             net.local(t_all.at[at(net.y * n_rows + net.z * n_slice, n_slice)], t_buf)]
    start(first)
    spread_up, spread_down = spread_of(0)
    fetches[0][0].arrived()
    spread_up.start()
    fetches[0][1].arrived()
    spread_down.start()
    spread_up.relay()
    spread_down.relay()
    spread_up.cross()
    spread_up.finish()
    start(loads[0][1])
    wait(first)
    per_part = 8 // PARTS

    h_rows, a_moves = {}, []
    for layer in range(layers):
        b = layer % 2
        h_ref, out_ref = rows_buf.at[b], rows_buf.at[1 - b]
        spreads, rows = None, None
        if layer > 0:
            rows = h_rows[layer] = RowGather(net, h_ref, h_all.at[layer - 1])
            rows.start()
            if layer < top:
                fetches[layer + 1][0].arrived()
                fetches[layer + 1][1].arrived()
                spreads = spread_of(layer + 1)
                start(spreads)
        loads[0][0].wait()
        wait(loads[0][1])

        @pl.loop(0, NY)
        def _(n):
            block = at(n * cols, cols)
            pre = jnp.dot(h_ref[...], wu[b, :, block], preferred_element_type=F32).astype(BF16)
            u_buf[layer, :, block] = pre
            act[:, block] = gelu_tanh(pre.astype(F32)).astype(BF16)

        exchange = ColumnExchange(net, act, a_all.at[layer])
        a_moves.append(exchange)
        if layer == 0:
            exchange.start()
            spread_down.cross()
            spread_down.finish()
            start(loads[1][1])
            fetches[1][0].arrived()
            fetches[1][1].arrived()
            spreads = spread_of(1)
            start(spreads)
        ring = z_ring(net, part, slots, out_ref)

        def down(n):
            part[:, at(n * tile, tile)] = jnp.dot(act[...], wd[b, :, at(n * tile, tile)], preferred_element_type=F32)

        loads[1][0].wait()
        wait(loads[1][1])
        for q in range(PARTS):
            pl.loop(q * per_part, (q + 1) * per_part)(down)
            ring.reduce_half(q)
        if layer == 0:
            for ahead in range(2, layers):
                fetches.append(fetch_of(ahead))
                start(fetches[ahead])
        else:
            exchange.start()
        for step in (1, 2, 3):
            ring.reduce_all(step)
        if spreads and layer > 0:
            spreads[0].relay()
            spreads[1].relay()
        for q in range(PARTS):
            value = ring.block(h_ref)(0, q)[...] + ring.total(q).astype(BF16)
            if layer == top:
                wide = value.shape[1]
                err = value.astype(F32) - t_buf[:, q * wide:(q + 1) * wide].astype(F32)
                value = (err / total_tokens).astype(BF16)
            ring.out(0, q)[...] = value
            ring.gather_half(q)
        if rows:
            rows.relay()
        if spreads and layer == 0:
            spreads[0].relay()
            spreads[1].relay()
        ring.gather_all(1)
        ring.gather_all(2)
        if spreads:
            spreads[0].cross()
            spreads[1].cross()
        ring.gather_all(3)
        if spreads:
            spreads[0].finish()
            spreads[1].finish()
            loads = up_loads(layer + 1), down_loads(layer + 1)
            for own, others in loads:
                own.start()
                start(others)
        if rows:
            rows.sent()
        exchange.sent()
        ring.arrived()
        ring.finish()
    for pair in fetches:
        pair[0].sent()
        pair[1].sent()

    def up_product(lo, hi):
        tall = up_part.shape[2]

        @pl.loop(lo, hi)
        def _(n):
            up_part[lax.div(n, 2), lax.rem(n, 2)] = lax.dot_general(
                h_in[:, at(n * tall, tall)], du_in[...], ROW_CONTRACT, preferred_element_type=F32)

    def down_product(lo, hi, g):
        @pl.loop(lo, hi)
        def _(n):
            block = at(n * tile, tile)
            value = lax.dot_general(a_in[...], g[:, block], ROW_CONTRACT, preferred_element_type=F32)
            down_part[:, :, :, block] = value.reshape(NX, 2, cols // 8, tile)

    def do(*actions):
        def job():
            for action in actions:
                action()
        return job

    reload, prev_rows, prev_up, prev_down, prev_a, prev_layer = {}, None, None, None, None, None
    for layer in reversed(range(layers)):
        b = layer % 2
        g_ref, out_ref = rows_buf.at[1 - b], rows_buf.at[b]
        if layer > 0:
            h_rows[layer].finish()
        a_moves[layer].arrived()
        h_load = net.local(x_all if layer == 0 else h_all.at[layer - 1], h_in)
        h_load.start()
        a_load = net.local(a_all.at[layer], a_in)
        if layer in reload:
            reload[layer][0][0].wait()
            wait(reload[layer][0][1])

        @pl.loop(0, NY)
        def _(n):
            block = at(n * cols, cols)
            d_act = lax.dot_general(g_ref[...], wd[b, block, :], COL_CONTRACT, preferred_element_type=F32)
            _, gelu_vjp = jax.vjp(gelu_tanh, u_buf[layer, :, block].astype(F32))
            dpre[:, block] = gelu_vjp(d_act)[0].astype(BF16)

        exchange = ColumnExchange(net, dpre, du_all.at[layer])
        exchange.start()
        du_load = net.local(du_all.at[layer], du_in)
        if layer == 0:
            break
        rows = RowGather(net, g_ref, g_all.at[layer])
        rows.start()
        if layer in reload:
            reload[layer][1][0].wait()
            wait(reload[layer][1][1])
        ring = z_ring(net, part, slots, out_ref)

        def back(n):
            part[:, at(n * tile, tile)] = lax.dot_general(
                dpre[...], wu[b, at(n * tile, tile), :], COL_CONTRACT, preferred_element_type=F32)

        for q in range(PARTS):
            pl.loop(q * per_part, (q + 1) * per_part)(back)
            ring.reduce_half(q)
        if layer >= 2:
            reload[layer - 2] = (down_loads(layer - 2), up_loads(layer - 2)) if layer > 2 else (down_loads(0),)
            for own, others in reload[layer - 2]:
                own.start()
                start(others)
        jobs = {name: [] for name in ("r1", "r2", "r3", "t", "g1", "g2", "g3")}
        up_sum = GradSum(net, up_part, up_sib, up_slots, grad_up.at[layer])
        down_sum = None
        if prev_down:
            jobs["r1"] += [prev_down.relay]
        if prev_up:
            jobs["r1"] += [prev_up.step]
        if prev_down:
            jobs["r2"] += [do(prev_down.finish, prev_down.end)]
        if prev_rows:
            down_sum = GradSum(net, down_part, down_sib, down_slots, grad_down.at[prev_layer])
            g_load = net.local(g_all.at[prev_layer], g_in)
            jobs["r1"] += [do(prev_rows.finish, g_load.start)]
            jobs["r2"] += [do(g_load.wait, prev_a.wait, functools.partial(down_product, 0, 2, g_in))]
            jobs["r2"] += [functools.partial(down_product, n, n + 2, g_in) for n in (2, 4)]
            jobs["r2"] += [do(functools.partial(down_product, 6, 8, g_in), down_sum.swap.start, a_load.start), prev_up.settle]
            jobs["r3"] += [down_sum.merge, prev_up.relay]
            jobs["t"] += [prev_up.finish]
            jobs["g1"] += [do(prev_up.end, down_sum.step)]
        else:
            jobs["r2"] += [a_load.start]
        jobs["r3"] += [do(exchange.sent, exchange.arrived, du_load.start)]
        jobs["g1"] += [do(h_load.wait, du_load.wait, functools.partial(up_product, 0, 2))]
        jobs["g1"] += [functools.partial(up_product, n, n + 2) for n in (2, 4)]
        jobs["g1"] += [do(functools.partial(up_product, 6, 8), up_sum.swap.start)]
        jobs["g2"] += [rows.relay, up_sum.merge]
        if down_sum:
            jobs["g3"] += [down_sum.settle]
        ring.reduce_all(1, jobs["r1"])
        ring.reduce_all(2, jobs["r2"])
        ring.reduce_all(3, jobs["r3"])
        for q in range(PARTS):
            total = ring.total(q)
            ring.out(0, q)[...] = (ring.block(g_ref)(0, q)[...].astype(F32) + total).astype(BF16)
            ring.gather_half(q)
        for job in jobs["t"]:
            job()
        ring.gather_all(1, jobs["g1"])
        ring.gather_all(2, jobs["g2"])
        ring.gather_all(3, jobs["g3"])
        rows.sent()
        ring.arrived()
        ring.finish()
        prev_rows, prev_up, prev_down, prev_a, prev_layer = rows, up_sum, down_sum, a_load, layer

    wide = width // PARTS

    def piece_of(ref, q):
        return ref.at[(slice(None),) * (len(ref.shape) - 1) + (slice(q * wide, (q + 1) * wide),)]

    pieces = [RowGather(net, piece_of(g_ref, q), piece_of(g_last, q)) for q in range(PARTS)]
    pieces[0].start()
    pieces[1].start()
    if prev_down:
        prev_down.relay()
    prev_up.step()
    prev_rows.finish()
    g_load = net.local(g_all.at[prev_layer], g_in)
    g_load.start()
    if prev_down:
        prev_down.finish()
        prev_down.end()
    g_load.wait()
    prev_a.wait()
    down_sum = GradSum(net, down_part, down_sib, down_slots, grad_down.at[prev_layer])
    down_product(0, 8, g_in)
    down_sum.swap.start()
    a_load.start()
    prev_up.settle()
    exchange.sent()
    exchange.arrived()
    du_load.start()
    down_sum.merge()
    prev_up.relay()
    pieces[0].relay()
    pieces[2].start()
    prev_up.finish()
    down_sum.step()
    prev_up.end()
    h_load.wait()
    du_load.wait()
    up_sum = GradSum(net, up_part, up_sib, up_slots, grad_up.at[0])
    up_product(0, 8)
    up_sum.swap.start()
    pieces[1].relay()
    pieces[3].start()
    up_sum.merge()
    down_sum.settle()
    pieces[2].relay()
    up_sum.step()
    down_sum.relay()
    pieces[3].relay()
    up_sum.settle()
    down_sum.finish()
    down_sum.end()
    a_load.wait()
    sums = []
    for q in range(PARTS):
        pieces[q].sent()
        pieces[q].finish()
        down_product(q * per_part, (q + 1) * per_part, g_last)
        sums.append(GradSum(net, piece_of(down_part, q), piece_of(down_sib, q), piece_of(down_slots, q), piece_of(grad_down.at[0], q)))
        sums[q].swap.start()
        if q == 1:
            up_sum.relay()
        if q == 2:
            sums[0].step()
        sums[q].merge()
    up_sum.finish()
    sums[1].step()
    sums[0].settle()
    sums[2].step()
    sums[1].settle()
    sums[3].step()
    sums[2].settle()
    sums[0].relay()
    sums[3].settle()
    for q in (1, 2, 3):
        sums[q].relay()
    up_sum.end()
    for q in range(PARTS):
        sums[q].finish()
    for q in range(PARTS):
        sums[q].end()


def local_step(hidden, targets, w_up, w_down, n_dp):
    layers, width, cols = w_up.shape
    tokens = hidden.shape[0]
    rows, inner, piece = tokens // NY, cols * NY, width // n_dp
    up_shape, down_shape = (NX, 2, width // 8, cols), (NX, 2, cols // 8, width)

    def out(dtype, *shape):
        return jax.ShapeDtypeStruct(shape, dtype)

    outs = [out(F32, layers, *up_shape), out(F32, layers, *down_shape),
            out(BF16, layers, NY - 1, width, cols), out(BF16, layers, n_dp, (NY - 1) * cols, piece),
            out(BF16, layers - 1, tokens, width), out(BF16, layers, tokens, cols),
            out(BF16, layers, tokens, width), out(BF16, layers, tokens, cols)]

    def sum_scratch(shape):
        return [pltpu.VMEM(shape, F32), pltpu.VMEM((NX, *shape[2:]), F32), pltpu.VMEM((6, shape[2] // 2, shape[3]), F32)]

    scratch = [pltpu.VMEM((2, width, inner), BF16), pltpu.VMEM((2, inner, width), BF16), pltpu.VMEM((2, rows, width), BF16),
               pltpu.VMEM((layers, rows, inner), BF16), pltpu.VMEM((rows, inner), BF16), pltpu.VMEM((rows, inner), BF16),
               pltpu.VMEM((rows, width), F32), pltpu.VMEM((7 * PARTS, rows // NZ, width // PARTS), F32),
               pltpu.VMEM((layers, NY - 1, piece, cols), BF16), pltpu.VMEM((layers, (NY - 1) * cols, piece), BF16),
               *sum_scratch(up_shape), *sum_scratch(down_shape),
               pltpu.VMEM((tokens, cols), BF16), pltpu.VMEM((tokens, width), BF16), pltpu.VMEM((tokens, width), BF16), pltpu.VMEM((tokens, cols), BF16),
               pltpu.VMEM((tokens, width), BF16), pltpu.VMEM((rows // NZ, width), BF16),
               pltpu.SemaphoreType.DMA((COPIES,)), pltpu.SemaphoreType.DMA((COPIES,)), pltpu.SemaphoreType.DMA((LOCALS,))]
    up, down = pl.pallas_call(
        functools.partial(step_kernel, layers, tokens * n_dp), out_shape=outs, in_specs=[ANY] * 4,
        out_specs=[ANY] * len(outs), scratch_shapes=scratch, name="step",
        compiler_params=pltpu.CompilerParams(collective_id=0, has_side_effects=True, vmem_limit_bytes=60 * 1024 * 1024),
    )(hidden, targets, w_up, w_down)[:2]
    return up.reshape(layers, width, cols), down.reshape(layers, cols, width)


def solution(mesh):
    n_dp = mesh.shape["dp"]

    def grad_step(hidden_in, targets, w_up, w_down):
        step_fn = functools.partial(local_step, n_dp=n_dp)
        mapped = jax.shard_map(step_fn, mesh=mesh, in_specs=(P("dp", None), P("dp", None), P(None, None, "tp"), P(None, "tp", None)), out_specs=(P(None, None, "tp"), P(None, "tp", None)), check_vma=False)
        return mapped(hidden_in, targets, w_up, w_down)

    return grad_step
```

```python
import functools
import jax
import jax.numpy as jnp
from jax import lax
from jax.experimental import pallas as pl
from jax.experimental.pallas import tpu as pltpu
from jax.sharding import PartitionSpec as P

NZ, NY, NX = 8, 4, 4
COPIES, LOCALS = 832, 160
PARTS = 4
ROW_CONTRACT = (((0,), (0,)), ((), ()))
COL_CONTRACT = (((1,), (1,)), ((), ()))
Z_CHAINS = tuple(chain for q in range(PARTS) for chain in ((q % 2, q, 4), (1 - q % 2, q, 3)))
X_CHAINS = ((0, 0, 2), (1, 0, 1), (1, 1, 2), (0, 1, 1))
ANY = pl.BlockSpec(memory_space=pl.ANY)
BF16, F32 = jnp.bfloat16, jnp.float32


def gelu_tanh(value):
    return jax.nn.gelu(value, approximate=True)


def at(start, size):
    return pl.ds(pl.multiple_of(start, size), size)


class Net:
    def __init__(self, send_sem, recv_sem, local_sem):
        tp, dp = lax.axis_index("tp"), lax.axis_index("dp")
        self.z, self.y = lax.div(tp, NY), lax.rem(tp, NY)
        self.x, self.c = lax.div(dp, 2), lax.rem(dp, 2)
        self.other = 1 - self.c
        self.send_sem, self.recv_sem, self.local_sem = send_sem, recv_sem, local_sem
        self.n_copies = self.n_locals = 0
        self.known = {}

    def near(self, axis, amount):
        size = {"x": NX, "y": NY, "z": NZ}[axis]
        key = axis, amount % size
        if key not in self.known:
            here = getattr(self, axis)
            self.known[key] = lax.rem(here + key[1], size) if key[1] else here
        return self.known[key]

    def span(self, axis, amount, rows):
        key = axis, amount % {"x": NX, "y": NY, "z": NZ}[axis], rows
        if key not in self.known:
            self.known[key] = at(self.near(axis, amount) * rows, rows)
        return self.known[key]

    def block(self, dx):
        key = "block", dx % NX
        if key not in self.known:
            self.known[key] = self.near("x", dx) * 2 + self.c
        return self.known[key]

    def device(self, dz=0, dy=0, dx=0, other_core=False):
        key = "device", dz % NZ, dy % NY, dx % NX, other_core
        if key not in self.known:
            c = self.other if other_core else self.c
            self.known[key] = {"tp": self.near("z", dz) * NY + self.near("y", dy), "dp": self.near("x", dx) * 2 + c}
        return self.known[key]

    def barrier(self):
        peers = [self.device(dy=s) for s in (1, 2, 3)] + [self.device(dz=s) for s in (1, -1)]
        peers += [self.device(dx=s) for s in (1, -1)] + [self.device(other_core=True)]
        sem = pltpu.get_barrier_semaphore()
        for peer in peers:
            pl.semaphore_signal(sem, inc=1, device_id=peer, device_id_type=pl.DeviceIdType.MESH)
        pl.semaphore_wait(sem, len(peers))

    def copy(self, src, dst, **where):
        index = self.n_copies
        self.n_copies += 1
        return pltpu.make_async_remote_copy(
            src_ref=src, dst_ref=dst, send_sem=self.send_sem.at[index], recv_sem=self.recv_sem.at[index],
            device_id=self.device(**where), device_id_type=pl.DeviceIdType.MESH)

    def local(self, src, dst):
        index = self.n_locals
        self.n_locals += 1
        return pltpu.make_async_copy(src, dst, self.local_sem.at[index])


class RowGather:
    def __init__(self, net, block, out):
        rows = block.shape[0]
        half = rows // 2
        own = out.at[net.span("y", 0, rows)]
        lower, upper = out.at[net.span("y", -1, rows)].at[0:half], out.at[net.span("y", 1, rows)].at[half:rows]
        self.local = net.local(block, own)
        self.first = [net.copy(block, own, dy=1), net.copy(block, own, dy=-1)]
        self.second = [net.copy(lower, lower, dy=1), net.copy(upper, upper, dy=-1)]

    def start(self):
        self.local.start()
        for copy in self.first:
            copy.start()

    def relay(self):
        for copy, onward in zip(self.first, self.second):
            copy.wait_recv()
            onward.start()

    def sent(self):
        self.local.wait()
        for copy in self.first:
            copy.wait_send()

    def finish(self):
        for copy in self.second:
            copy.wait()


class ColumnExchange:
    def __init__(self, net, block, out):
        rows, cols = block.shape[0], block.shape[1] // NY
        own = out.at[net.span("y", 0, rows)]
        self.local = net.local(block.at[:, 0:cols], own)
        self.copies = [net.copy(block.at[:, s * cols:(s + 1) * cols], own, dy=s) for s in (1, 3, 2)]

    def start(self):
        self.local.start()
        for copy in self.copies:
            copy.start()

    def sent(self):
        self.local.wait()
        for copy in self.copies:
            copy.wait_send()

    def arrived(self):
        for copy in self.copies:
            copy.wait_recv()


class PieceFetch:
    def __init__(self, net, piece, slot):
        self.copies = [net.copy(piece, slot(NY - s - 1), dy=s) for s in (1, 3, 2)]

    def start(self):
        for copy in self.copies:
            copy.start()

    def arrived(self):
        for copy in self.copies:
            copy.wait_recv()

    def sent(self):
        for copy in self.copies:
            copy.wait_send()


class PieceSpread:
    def __init__(self, net, held, view):
        own = view(0, None)
        self.local = net.local(held, own)
        self.first = [net.copy(held, own, dx=d) for d in (1, -1)]
        self.second = [net.copy(view(-d, half), view(-d, half), dx=d) for half, d in ((0, 1), (1, -1))]
        self.across = [net.copy(held, own, other_core=True)]
        self.across += [net.copy(view(d, None), view(d, None), other_core=True) for d in (-1, 1, 2)]

    def start(self):
        for copy in (self.local, *self.first, self.across[0]):
            copy.start()

    def relay(self):
        for first, second, across in zip(self.first, self.second, self.across[1:3]):
            first.wait_recv()
            second.start()
            across.start()

    def cross(self):
        for copy in self.second:
            copy.wait_recv()
        self.across[3].start()

    def finish(self):
        self.local.wait()
        for copy in (*self.first, *self.second):
            copy.wait_send()
        for copy in self.across:
            copy.wait()


class Ring:
    def __init__(self, net, axis, chains, part, slot, out):
        self.net, self.axis, self.chains = net, axis, chains
        self.part, self.slot, self.out = part, slot, out
        self.copies, self.last = [], {}

    def owner(self, direction, amount):
        return amount if direction == 0 else -amount

    def send(self, chain, src, dst):
        direction = self.chains[chain][0]
        copy = self.net.copy(src, dst, **{"d" + self.axis: 1 if direction == 0 else -1})
        copy.start()
        self.copies.append(copy)
        self.last[chain] = copy

    def reduce(self, chain, step):
        direction, half, hops = self.chains[chain]
        if step >= hops:
            return
        mine = self.part(self.owner(direction, hops - step), half)
        if step > 0:
            self.last[chain].wait_recv()
            mine[...] = mine[...] + self.slot(chain, step - 1)[...]
        self.send(chain, mine, self.slot(chain, step))

    def reduce_half(self, half):
        for chain, (_, h, _) in enumerate(self.chains):
            if h == half:
                self.reduce(chain, 0)

    def reduce_all(self, step, jobs=()):
        self.events(self.reduce, step, jobs)

    def events(self, action, step, jobs):
        jobs = list(jobs)
        for chain, (_, _, hops) in enumerate(self.chains):
            if step < hops:
                action(chain, step)
                if jobs:
                    jobs.pop(0)()
        for job in jobs:
            job()

    def total(self, half):
        value = self.part(0, half)[...]
        for chain, (_, h, hops) in enumerate(self.chains):
            if h == half:
                self.last[chain].wait_recv()
                value = value + self.slot(chain, hops - 1)[...]
        return value

    def gather(self, chain, step, first=None):
        direction, half, hops = self.chains[chain]
        if step >= hops:
            return
        if step > 0:
            self.last[chain].wait_recv()
        held = self.out(self.owner(direction, -step), half)
        self.send(chain, held if first is None else first, held)

    def gather_half(self, half):
        for chain, (_, h, _) in enumerate(self.chains):
            if h == half:
                self.gather(chain, 0)

    def gather_all(self, step, jobs=()):
        self.events(self.gather, step, jobs)

    def arrived(self):
        for copy in self.last.values():
            copy.wait_recv()

    def finish(self):
        for copy in self.copies:
            copy.wait_send()


def slot_index(chains, chain, step):
    return sum(hops for _, _, hops in chains[:chain]) + step


def z_ring(net, part, slots, out):
    rows, cols = part.shape[0] // NZ, part.shape[1] // PARTS

    def block(ref):
        return lambda owner, half: ref.at[net.span("z", owner, rows), half * cols:(half + 1) * cols]

    ring = Ring(net, "z", Z_CHAINS, block(part), lambda chain, step: slots.at[slot_index(Z_CHAINS, chain, step)], block(out))
    ring.block = block
    return ring


class GradSum:
    def __init__(self, net, part, sib, slots, out):
        self.net, self.mine, self.sib, self.out = net, part, sib, out
        half_rows = part.shape[2] // 2

        def block(ref):
            return lambda owner, half: ref.at[net.near("x", owner), net.c, half * half_rows:(half + 1) * half_rows]

        self.ring = Ring(net, "x", X_CHAINS, block(part), lambda chain, step: slots.at[slot_index(X_CHAINS, chain, step)], block(out))
        self.swap = net.copy(part.at[:, net.other], sib, other_core=True)
        self.across, self.local = [], []

    def merge(self):
        c = self.net.c
        self.swap.wait_recv()
        for k in range(NX):
            self.mine[k, c] = self.mine[k, c] + self.sib[k]
        for half in (0, 1):
            self.ring.reduce_half(half)

    def step(self):
        self.ring.reduce_all(1)

    def cross(self, src, dst):
        copy = self.net.copy(src, dst, other_core=True)
        copy.start()
        self.across.append(copy)

    def settle(self):
        for half in (0, 1):
            own = self.ring.part(0, half)
            own[...] = self.ring.total(half)
            for chain, (_, h, _) in enumerate(X_CHAINS):
                if h == half:
                    self.ring.gather(chain, 0, own)
        x, c = self.net.x, self.net.c
        self.local = self.net.local(self.mine.at[x, c], self.out.at[x, c])
        self.local.start()
        self.cross(self.mine.at[x, c], self.out.at[x, c])

    def relay(self):
        self.ring.gather_all(1)

    def finish(self):
        self.ring.arrived()
        for dx in (1, -1, 2):
            held = self.out.at[self.net.near("x", dx), self.net.c]
            self.cross(held, held)
        self.local.wait()
        self.swap.wait_send()
        self.ring.finish()

    def end(self):
        for copy in self.across:
            copy.wait()


def take(refs, count):
    taken = refs[:count]
    del refs[:count]
    return taken if count > 1 else taken[0]


def step_kernel(layers, total_tokens, *refs):
    refs = list(refs)
    x_all, t_all, w_up, w_down = take(refs, 4)
    grad_up, grad_down = take(refs, 2)
    all_up, all_down, h_all, a_all, g_all, du_all = take(refs, 6)
    wu, wd, rows_buf, u_buf, act, dpre, part, slots = take(refs, 8)
    held_up, held_down = take(refs, 2)
    up_part, up_sib, up_slots, down_part, down_sib, down_slots = take(refs, 6)
    a_in, g_in, h_in, du_in, g_last, t_buf = take(refs, 6)
    net = Net(*refs)
    top = layers - 1
    width, hidden = wu.shape[1], wu.shape[2]
    cols = hidden // NY
    piece = held_up.shape[2]
    tile = width // 8
    pieces_at = {dx: at(net.block(dx) * piece, piece) for dx in range(NX)}

    def start(copies):
        for copy in copies:
            copy.start()

    def wait(copies):
        for copy in copies:
            copy.wait()

    own_piece = pieces_at[0]

    def fetch_of(layer):
        return (PieceFetch(net, w_up.at[layer, own_piece], lambda slot: held_up.at[layer, slot]),
                PieceFetch(net, w_down.at[layer, :, own_piece], lambda slot: held_down.at[layer, slot * cols:(slot + 1) * cols]))

    def spread_of(layer):
        def up_view(dx, half):
            whole = all_up.at[layer, :, pieces_at[dx % NX]]
            return whole if half is None else whole.at[:, half * (piece // 2):(half + 1) * (piece // 2)]

        def down_view(dx, half):
            index, tall = net.block(dx), 3 * cols
            if half is None:
                return all_down.at[layer, index]
            return all_down.at[layer, index, half * (tall // 2):(half + 1) * (tall // 2)]

        return PieceSpread(net, held_up.at[layer], up_view), PieceSpread(net, held_down.at[layer], down_view)

    def up_loads(layer):
        b = layer % 2
        own = net.local(w_up.at[layer], wu.at[b, :, 0:cols])
        return own, [net.local(all_up.at[layer, s], wu.at[b, :, (s + 1) * cols:(s + 2) * cols]) for s in range(NY - 1)]

    def down_loads(layer):
        b = layer % 2
        own = net.local(w_down.at[layer], wd.at[b, 0:cols])
        return own, [net.local(all_down.at[layer, n], wd.at[b, cols:, n * piece:(n + 1) * piece]) for n in range(all_down.shape[1])]

    net.barrier()
    fetches = [fetch_of(0)]
    start(fetches[0])
    for ahead in range(1, layers - 1):
        fetches.append(fetch_of(ahead))
        start(fetches[ahead])
    loads = up_loads(0), down_loads(0)
    loads[0][0].start()
    loads[1][0].start()
    n_rows = rows_buf.shape[1]
    n_slice = n_rows // NZ
    first = [net.local(x_all.at[at(net.y * n_rows, n_rows)], rows_buf.at[0]),
             net.local(t_all.at[at(net.y * n_rows + net.z * n_slice, n_slice)], t_buf)]
    start(first)
    spread_up, spread_down = spread_of(0)
    fetches[0][0].arrived()
    spread_up.start()
    fetches[0][1].arrived()
    spread_down.start()
    spread_up.relay()
    spread_down.relay()
    spread_up.cross()
    spread_up.finish()
    start(loads[0][1])
    wait(first)
    per_part = 8 // PARTS

    h_rows, a_moves = {}, []
    for layer in range(layers):
        b = layer % 2
        h_ref, out_ref = rows_buf.at[b], rows_buf.at[1 - b]
        spreads, rows = None, None
        if layer > 0:
            rows = h_rows[layer] = RowGather(net, h_ref, h_all.at[layer - 1])
            rows.start()
            if layer < top:
                fetches[layer + 1][0].arrived()
                fetches[layer + 1][1].arrived()
                spreads = spread_of(layer + 1)
                start(spreads)
        loads[0][0].wait()
        wait(loads[0][1])

        @pl.loop(0, NY)
        def _(n):
            block = at(n * cols, cols)
            pre = jnp.dot(h_ref[...], wu[b, :, block], preferred_element_type=F32).astype(BF16)
            u_buf[layer, :, block] = pre
            act[:, block] = gelu_tanh(pre.astype(F32)).astype(BF16)

        exchange = ColumnExchange(net, act, a_all.at[layer])
        a_moves.append(exchange)
        if layer == 0:
            exchange.start()
            spread_down.cross()
            spread_down.finish()
            start(loads[1][1])
            fetches[1][0].arrived()
            fetches[1][1].arrived()
            spreads = spread_of(1)
            start(spreads)
        ring = z_ring(net, part, slots, out_ref)

        def down(n):
            part[:, at(n * tile, tile)] = jnp.dot(act[...], wd[b, :, at(n * tile, tile)], preferred_element_type=F32)

        loads[1][0].wait()
        wait(loads[1][1])
        for q in range(PARTS):
            pl.loop(q * per_part, (q + 1) * per_part)(down)
            ring.reduce_half(q)
        if layer == 0:
            fetches.append(fetch_of(top))
            start(fetches[top])
        else:
            exchange.start()
        for step in (1, 2, 3):
            ring.reduce_all(step)
        if spreads and layer > 0:
            spreads[0].relay()
            spreads[1].relay()
        for q in range(PARTS):
            value = ring.block(h_ref)(0, q)[...] + ring.total(q).astype(BF16)
            if layer == top:
                wide = value.shape[1]
                err = value.astype(F32) - t_buf[:, q * wide:(q + 1) * wide].astype(F32)
                value = (err / total_tokens).astype(BF16)
            ring.out(0, q)[...] = value
            ring.gather_half(q)
        if rows:
            rows.relay()
        if spreads and layer == 0:
            spreads[0].relay()
            spreads[1].relay()
        ring.gather_all(1)
        ring.gather_all(2)
        if spreads:
            spreads[0].cross()
            spreads[1].cross()
        ring.gather_all(3)
        if spreads:
            spreads[0].finish()
            spreads[1].finish()
            loads = up_loads(layer + 1), down_loads(layer + 1)
            for own, others in loads:
                own.start()
                start(others)
        if rows:
            rows.sent()
        exchange.sent()
        ring.arrived()
        ring.finish()
    for pair in fetches:
        pair[0].sent()
        pair[1].sent()

    def up_product(lo, hi):
        tall = up_part.shape[2]

        @pl.loop(lo, hi)
        def _(n):
            up_part[lax.div(n, 2), lax.rem(n, 2)] = lax.dot_general(
                h_in[:, at(n * tall, tall)], du_in[...], ROW_CONTRACT, preferred_element_type=F32)

    def down_product(lo, hi, g):
        @pl.loop(lo, hi)
        def _(n):
            block = at(n * tile, tile)
            value = lax.dot_general(a_in[...], g[:, block], ROW_CONTRACT, preferred_element_type=F32)
            down_part[:, :, :, block] = value.reshape(NX, 2, cols // 8, tile)

    def do(*actions):
        def job():
            for action in actions:
                action()
        return job

    def piece_of(ref, q, count=PARTS):
        wide = ref.shape[-1] // count
        return ref.at[(slice(None),) * (len(ref.shape) - 1) + (slice(q * wide, (q + 1) * wide),)]

    reload, prev_rows, prev_up, prev_down, prev_a, prev_layer = {}, None, None, None, None, None
    for layer in reversed(range(layers)):
        b = layer % 2
        g_ref, out_ref = rows_buf.at[1 - b], rows_buf.at[b]
        if layer > 0:
            h_rows[layer].finish()
        a_moves[layer].arrived()
        h_load = net.local(x_all if layer == 0 else h_all.at[layer - 1], h_in)
        h_load.start()
        a_load = net.local(a_all.at[layer], a_in)
        if layer in reload:
            reload[layer][0][0].wait()
            wait(reload[layer][0][1])

        @pl.loop(0, NY)
        def _(n):
            block = at(n * cols, cols)
            d_act = lax.dot_general(g_ref[...], wd[b, block, :], COL_CONTRACT, preferred_element_type=F32)
            _, gelu_vjp = jax.vjp(gelu_tanh, u_buf[layer, :, block].astype(F32))
            dpre[:, block] = gelu_vjp(d_act)[0].astype(BF16)

        exchange = ColumnExchange(net, dpre, du_all.at[layer])
        exchange.start()
        du_load = net.local(du_all.at[layer], du_in)
        if layer == 0:
            break
        rows = [RowGather(net, piece_of(g_ref, k, 2), piece_of(g_all.at[layer], k, 2)) for k in (0, 1)]
        for gather in rows:
            gather.start()
        if layer in reload:
            reload[layer][1][0].wait()
            wait(reload[layer][1][1])
        ring = z_ring(net, part, slots, out_ref)

        def back(n):
            part[:, at(n * tile, tile)] = lax.dot_general(
                dpre[...], wu[b, at(n * tile, tile), :], COL_CONTRACT, preferred_element_type=F32)

        for q in range(PARTS):
            pl.loop(q * per_part, (q + 1) * per_part)(back)
            ring.reduce_half(q)
        if layer >= 2:
            reload[layer - 2] = (down_loads(layer - 2), up_loads(layer - 2)) if layer > 2 else (down_loads(0),)
            for own, others in reload[layer - 2]:
                own.start()
                start(others)
        jobs = {name: [] for name in ("r1", "r2", "r3", "t", "g1", "g2", "g3")}
        up_sum = GradSum(net, up_part, up_sib, up_slots, grad_up.at[layer])
        down_sum = None
        if prev_down:
            jobs["r1"] += [prev_down.relay]
        if prev_rows:
            down_sum = GradSum(net, down_part, down_sib, down_slots, grad_down.at[prev_layer])
            g_load = net.local(g_all.at[prev_layer], g_in)
            jobs["r1"] += [prev_up.settle, do(prev_rows[0].finish, prev_rows[1].finish, g_load.start)]
            if prev_down:
                jobs["r2"] += [do(prev_down.finish, prev_down.end)]
            jobs["r2"] += [do(g_load.wait, prev_a.wait, functools.partial(down_product, 0, 2, g_in))]
            jobs["r2"] += [functools.partial(down_product, n, n + 2, g_in) for n in (2, 4)]
            jobs["r2"] += [do(functools.partial(down_product, 6, 8, g_in), down_sum.swap.start, a_load.start), prev_up.relay]
        else:
            jobs["r2"] += [a_load.start]
        jobs["r3"] += [do(exchange.sent, exchange.arrived, du_load.start)]
        if prev_rows:
            jobs["r3"] += [down_sum.merge, prev_up.finish]
            jobs["t"] += [prev_up.end]
        jobs["t"] += [do(h_load.wait, du_load.wait, functools.partial(up_product, 0, 2))]
        jobs["t"] += [functools.partial(up_product, n, n + 2) for n in (2, 4)]
        jobs["t"] += [do(functools.partial(up_product, 6, 8), up_sum.swap.start), rows[0].relay]
        jobs["g1"] += [up_sum.merge]
        if down_sum:
            jobs["g1"] += [down_sum.step]
            jobs["g3"] += [down_sum.settle]
        jobs["g3"] += [up_sum.step]
        ring.reduce_all(1, jobs["r1"])
        ring.reduce_all(2, jobs["r2"])
        ring.reduce_all(3, jobs["r3"])
        for q in range(PARTS):
            total = ring.total(q)
            ring.out(0, q)[...] = (ring.block(g_ref)(0, q)[...].astype(F32) + total).astype(BF16)
            ring.gather_half(q)
            if q + 1 < PARTS:
                jobs["t"].pop(0)()
        for job in jobs["t"]:
            job()
        ring.gather_all(1, jobs["g1"])
        ring.gather_all(2, jobs["g2"])
        ring.gather_all(3, jobs["g3"])
        rows[1].relay()
        for gather in rows:
            gather.sent()
        ring.arrived()
        ring.finish()
        prev_rows, prev_up, prev_down, prev_a, prev_layer = rows, up_sum, down_sum, a_load, layer

    pieces = [RowGather(net, piece_of(g_ref, q), piece_of(g_last, q)) for q in range(PARTS)]
    pieces[0].start()
    pieces[1].start()
    if prev_down:
        prev_down.relay()
    prev_up.settle()
    for gather in prev_rows:
        gather.finish()
    g_load = net.local(g_all.at[prev_layer], g_in)
    g_load.start()
    if prev_down:
        prev_down.finish()
        prev_down.end()
    g_load.wait()
    prev_a.wait()
    down_sum = GradSum(net, down_part, down_sib, down_slots, grad_down.at[prev_layer])
    down_product(0, 8, g_in)
    down_sum.swap.start()
    a_load.start()
    prev_up.relay()
    exchange.sent()
    exchange.arrived()
    du_load.start()
    down_sum.merge()
    pieces[0].relay()
    pieces[2].start()
    prev_up.finish()
    prev_up.end()
    h_load.wait()
    du_load.wait()
    up_sum = GradSum(net, up_part, up_sib, up_slots, grad_up.at[0])
    up_product(0, 8)
    up_sum.swap.start()
    down_sum.step()
    pieces[1].relay()
    pieces[3].start()
    up_sum.merge()
    down_sum.settle()
    pieces[2].relay()
    up_sum.step()
    down_sum.relay()
    pieces[3].relay()
    up_sum.settle()
    down_sum.finish()
    down_sum.end()
    a_load.wait()
    sums = []
    for q in range(PARTS):
        pieces[q].sent()
        pieces[q].finish()
        down_product(q * per_part, (q + 1) * per_part, g_last)
        sums.append(GradSum(net, piece_of(down_part, q), piece_of(down_sib, q), piece_of(down_slots, q), piece_of(grad_down.at[0], q)))
        sums[q].swap.start()
        if q == 1:
            up_sum.relay()
        if q == 2:
            sums[0].step()
        sums[q].merge()
    up_sum.finish()
    sums[1].step()
    sums[0].settle()
    sums[2].step()
    sums[1].settle()
    sums[3].step()
    sums[2].settle()
    sums[0].relay()
    sums[3].settle()
    for q in (1, 2, 3):
        sums[q].relay()
    up_sum.end()
    for q in range(PARTS):
        sums[q].finish()
    for q in range(PARTS):
        sums[q].end()


def local_step(hidden, targets, w_up, w_down, n_dp):
    layers, width, cols = w_up.shape
    tokens = hidden.shape[0]
    rows, inner, piece = tokens // NY, cols * NY, width // n_dp
    up_shape, down_shape = (NX, 2, width // 8, cols), (NX, 2, cols // 8, width)

    def out(dtype, *shape):
        return jax.ShapeDtypeStruct(shape, dtype)

    outs = [out(F32, layers, *up_shape), out(F32, layers, *down_shape),
            out(BF16, layers, NY - 1, width, cols), out(BF16, layers, n_dp, (NY - 1) * cols, piece),
            out(BF16, layers - 1, tokens, width), out(BF16, layers, tokens, cols),
            out(BF16, layers, tokens, width), out(BF16, layers, tokens, cols)]

    def sum_scratch(shape):
        return [pltpu.VMEM(shape, F32), pltpu.VMEM((NX, *shape[2:]), F32), pltpu.VMEM((6, shape[2] // 2, shape[3]), F32)]

    scratch = [pltpu.VMEM((2, width, inner), BF16), pltpu.VMEM((2, inner, width), BF16), pltpu.VMEM((2, rows, width), BF16),
               pltpu.VMEM((layers, rows, inner), BF16), pltpu.VMEM((rows, inner), BF16), pltpu.VMEM((rows, inner), BF16),
               pltpu.VMEM((rows, width), F32), pltpu.VMEM((7 * PARTS, rows // NZ, width // PARTS), F32),
               pltpu.VMEM((layers, NY - 1, piece, cols), BF16), pltpu.VMEM((layers, (NY - 1) * cols, piece), BF16),
               *sum_scratch(up_shape), *sum_scratch(down_shape),
               pltpu.VMEM((tokens, cols), BF16), pltpu.VMEM((tokens, width), BF16), pltpu.VMEM((tokens, width), BF16), pltpu.VMEM((tokens, cols), BF16),
               pltpu.VMEM((tokens, width), BF16), pltpu.VMEM((rows // NZ, width), BF16),
               pltpu.SemaphoreType.DMA((COPIES,)), pltpu.SemaphoreType.DMA((COPIES,)), pltpu.SemaphoreType.DMA((LOCALS,))]
    up, down = pl.pallas_call(
        functools.partial(step_kernel, layers, tokens * n_dp), out_shape=outs, in_specs=[ANY] * 4,
        out_specs=[ANY] * len(outs), scratch_shapes=scratch, name="step",
        compiler_params=pltpu.CompilerParams(collective_id=0, has_side_effects=True, vmem_limit_bytes=60 * 1024 * 1024),
    )(hidden, targets, w_up, w_down)[:2]
    return up.reshape(layers, width, cols), down.reshape(layers, cols, width)


def solution(mesh):
    n_dp = mesh.shape["dp"]

    def grad_step(hidden_in, targets, w_up, w_down):
        step_fn = functools.partial(local_step, n_dp=n_dp)
        mapped = jax.shard_map(step_fn, mesh=mesh, in_specs=(P("dp", None), P("dp", None), P(None, None, "tp"), P(None, "tp", None)), out_specs=(P(None, None, "tp"), P(None, "tp", None)), check_vma=False)
        return mapped(hidden_in, targets, w_up, w_down)

    return grad_step
```

```python
import functools
import jax
import jax.numpy as jnp
from jax import lax
from jax.experimental import pallas as pl
from jax.experimental.pallas import tpu as pltpu
from jax.sharding import PartitionSpec as P

NZ, NY, NX = 8, 4, 4
COPIES, LOCALS = 832, 160
PARTS = 4
ROW_CONTRACT = (((0,), (0,)), ((), ()))
COL_CONTRACT = (((1,), (1,)), ((), ()))
Z_CHAINS = tuple(chain for q in range(PARTS) for chain in ((q % 2, q, 4), (1 - q % 2, q, 3)))
X_CHAINS = ((0, 0, 2), (1, 0, 1), (1, 1, 2), (0, 1, 1))
ANY = pl.BlockSpec(memory_space=pl.ANY)
BF16, F32 = jnp.bfloat16, jnp.float32


def gelu_tanh(value):
    return jax.nn.gelu(value, approximate=True)


def at(start, size):
    return pl.ds(pl.multiple_of(start, size), size)


class Net:
    def __init__(self, send_sem, recv_sem, local_sem):
        tp, dp = lax.axis_index("tp"), lax.axis_index("dp")
        self.z, self.y = lax.div(tp, NY), lax.rem(tp, NY)
        self.x, self.c = lax.div(dp, 2), lax.rem(dp, 2)
        self.other = 1 - self.c
        self.send_sem, self.recv_sem, self.local_sem = send_sem, recv_sem, local_sem
        self.n_copies = self.n_locals = 0
        self.known = {}

    def near(self, axis, amount):
        size = {"x": NX, "y": NY, "z": NZ}[axis]
        key = axis, amount % size
        if key not in self.known:
            here = getattr(self, axis)
            self.known[key] = lax.rem(here + key[1], size) if key[1] else here
        return self.known[key]

    def span(self, axis, amount, rows):
        key = axis, amount % {"x": NX, "y": NY, "z": NZ}[axis], rows
        if key not in self.known:
            self.known[key] = at(self.near(axis, amount) * rows, rows)
        return self.known[key]

    def block(self, dx):
        key = "block", dx % NX
        if key not in self.known:
            self.known[key] = self.near("x", dx) * 2 + self.c
        return self.known[key]

    def device(self, dz=0, dy=0, dx=0, other_core=False):
        key = "device", dz % NZ, dy % NY, dx % NX, other_core
        if key not in self.known:
            c = self.other if other_core else self.c
            self.known[key] = {"tp": self.near("z", dz) * NY + self.near("y", dy), "dp": self.near("x", dx) * 2 + c}
        return self.known[key]

    def barrier(self):
        peers = [self.device(dy=s) for s in (1, 2, 3)] + [self.device(dz=s) for s in (1, -1)]
        peers += [self.device(dx=s) for s in (1, -1)] + [self.device(other_core=True)]
        sem = pltpu.get_barrier_semaphore()
        for peer in peers:
            pl.semaphore_signal(sem, inc=1, device_id=peer, device_id_type=pl.DeviceIdType.MESH)
        pl.semaphore_wait(sem, len(peers))

    def copy(self, src, dst, **where):
        index = self.n_copies
        self.n_copies += 1
        return pltpu.make_async_remote_copy(
            src_ref=src, dst_ref=dst, send_sem=self.send_sem.at[index], recv_sem=self.recv_sem.at[index],
            device_id=self.device(**where), device_id_type=pl.DeviceIdType.MESH)

    def local(self, src, dst):
        index = self.n_locals
        self.n_locals += 1
        return pltpu.make_async_copy(src, dst, self.local_sem.at[index])


class RowGather:
    def __init__(self, net, block, out):
        rows = block.shape[0]
        half = rows // 2
        own = out.at[net.span("y", 0, rows)]
        lower, upper = out.at[net.span("y", -1, rows)].at[0:half], out.at[net.span("y", 1, rows)].at[half:rows]
        self.local = net.local(block, own)
        self.first = [net.copy(block, own, dy=1), net.copy(block, own, dy=-1)]
        self.second = [net.copy(lower, lower, dy=1), net.copy(upper, upper, dy=-1)]

    def start(self):
        self.local.start()
        for copy in self.first:
            copy.start()

    def relay(self):
        for copy, onward in zip(self.first, self.second):
            copy.wait_recv()
            onward.start()

    def sent(self):
        self.local.wait()
        for copy in self.first:
            copy.wait_send()

    def finish(self):
        for copy in self.second:
            copy.wait()


class ColumnExchange:
    def __init__(self, net, block, out):
        rows, cols = block.shape[0], block.shape[1] // NY
        own = out.at[net.span("y", 0, rows)]
        self.local = net.local(block.at[:, 0:cols], own)
        self.copies = [net.copy(block.at[:, s * cols:(s + 1) * cols], own, dy=s) for s in (1, 3, 2)]

    def start(self):
        self.local.start()
        for copy in self.copies:
            copy.start()

    def sent(self):
        self.local.wait()
        for copy in self.copies:
            copy.wait_send()

    def arrived(self):
        for copy in self.copies:
            copy.wait_recv()


class PieceFetch:
    def __init__(self, net, piece, slot):
        self.copies = [net.copy(piece, slot(NY - s - 1), dy=s) for s in (1, 3, 2)]

    def start(self):
        for copy in self.copies:
            copy.start()

    def arrived(self):
        for copy in self.copies:
            copy.wait_recv()

    def sent(self):
        for copy in self.copies:
            copy.wait_send()


class PieceSpread:
    def __init__(self, net, held, view):
        own = view(0, None)
        self.local = net.local(held, own)
        self.first = [net.copy(held, own, dx=d) for d in (1, -1)]
        self.second = [net.copy(view(-d, half), view(-d, half), dx=d) for half, d in ((0, 1), (1, -1))]
        self.across = [net.copy(held, own, other_core=True)]
        self.across += [net.copy(view(d, None), view(d, None), other_core=True) for d in (-1, 1, 2)]

    def start(self):
        for copy in (self.local, *self.first, self.across[0]):
            copy.start()

    def relay(self):
        for first, second, across in zip(self.first, self.second, self.across[1:3]):
            first.wait_recv()
            second.start()
            across.start()

    def cross(self):
        for copy in self.second:
            copy.wait_recv()
        self.across[3].start()

    def finish(self):
        self.local.wait()
        for copy in (*self.first, *self.second):
            copy.wait_send()
        for copy in self.across:
            copy.wait()


class Ring:
    def __init__(self, net, axis, chains, part, slot, out):
        self.net, self.axis, self.chains = net, axis, chains
        self.part, self.slot, self.out = part, slot, out
        self.copies, self.last = [], {}

    def owner(self, direction, amount):
        return amount if direction == 0 else -amount

    def send(self, chain, src, dst):
        direction = self.chains[chain][0]
        copy = self.net.copy(src, dst, **{"d" + self.axis: 1 if direction == 0 else -1})
        copy.start()
        self.copies.append(copy)
        self.last[chain] = copy

    def reduce(self, chain, step):
        direction, half, hops = self.chains[chain]
        if step >= hops:
            return
        mine = self.part(self.owner(direction, hops - step), half)
        if step > 0:
            self.last[chain].wait_recv()
            mine[...] = mine[...] + self.slot(chain, step - 1)[...]
        self.send(chain, mine, self.slot(chain, step))

    def reduce_half(self, half):
        for chain, (_, h, _) in enumerate(self.chains):
            if h == half:
                self.reduce(chain, 0)

    def reduce_all(self, step, jobs=()):
        self.events(self.reduce, step, jobs)

    def events(self, action, step, jobs):
        jobs = list(jobs)
        for chain, (_, _, hops) in enumerate(self.chains):
            if step < hops:
                action(chain, step)
                if jobs:
                    jobs.pop(0)()
        for job in jobs:
            job()

    def total(self, half):
        value = self.part(0, half)[...]
        for chain, (_, h, hops) in enumerate(self.chains):
            if h == half:
                self.last[chain].wait_recv()
                value = value + self.slot(chain, hops - 1)[...]
        return value

    def gather(self, chain, step, first=None):
        direction, half, hops = self.chains[chain]
        if step >= hops:
            return
        if step > 0:
            self.last[chain].wait_recv()
        held = self.out(self.owner(direction, -step), half)
        self.send(chain, held if first is None else first, held)

    def gather_half(self, half):
        for chain, (_, h, _) in enumerate(self.chains):
            if h == half:
                self.gather(chain, 0)

    def gather_all(self, step, jobs=()):
        self.events(self.gather, step, jobs)

    def arrived(self):
        for copy in self.last.values():
            copy.wait_recv()

    def finish(self):
        for copy in self.copies:
            copy.wait_send()


def slot_index(chains, chain, step):
    return sum(hops for _, _, hops in chains[:chain]) + step


def z_ring(net, part, slots, out):
    rows, cols = part.shape[0] // NZ, part.shape[1] // PARTS

    def block(ref):
        return lambda owner, half: ref.at[net.span("z", owner, rows), half * cols:(half + 1) * cols]

    ring = Ring(net, "z", Z_CHAINS, block(part), lambda chain, step: slots.at[slot_index(Z_CHAINS, chain, step)], block(out))
    ring.block = block
    return ring


class GradSum:
    def __init__(self, net, part, sib, slots, out):
        self.net, self.mine, self.sib, self.out = net, part, sib, out
        half_rows = part.shape[2] // 2

        def block(ref):
            return lambda owner, half: ref.at[net.near("x", owner), net.c, half * half_rows:(half + 1) * half_rows]

        self.ring = Ring(net, "x", X_CHAINS, block(part), lambda chain, step: slots.at[slot_index(X_CHAINS, chain, step)], block(out))
        self.swap = net.copy(part.at[:, net.other], sib, other_core=True)
        self.across, self.local = [], []

    def merge(self):
        c = self.net.c
        self.swap.wait_recv()
        for k in range(NX):
            self.mine[k, c] = self.mine[k, c] + self.sib[k]
        for half in (0, 1):
            self.ring.reduce_half(half)

    def step(self):
        self.ring.reduce_all(1)

    def cross(self, src, dst):
        copy = self.net.copy(src, dst, other_core=True)
        copy.start()
        self.across.append(copy)

    def settle(self):
        for half in (0, 1):
            own = self.ring.part(0, half)
            own[...] = self.ring.total(half)
            for chain, (_, h, _) in enumerate(X_CHAINS):
                if h == half:
                    self.ring.gather(chain, 0, own)
        x, c = self.net.x, self.net.c
        self.local = self.net.local(self.mine.at[x, c], self.out.at[x, c])
        self.local.start()
        self.cross(self.mine.at[x, c], self.out.at[x, c])

    def relay(self):
        self.ring.gather_all(1)

    def finish(self):
        self.ring.arrived()
        for dx in (1, -1, 2):
            held = self.out.at[self.net.near("x", dx), self.net.c]
            self.cross(held, held)
        self.local.wait()
        self.swap.wait_send()
        self.ring.finish()

    def end(self):
        for copy in self.across:
            copy.wait()


def take(refs, count):
    taken = refs[:count]
    del refs[:count]
    return taken if count > 1 else taken[0]


def step_kernel(layers, total_tokens, *refs):
    refs = list(refs)
    x_all, t_all, w_up, w_down = take(refs, 4)
    grad_up, grad_down = take(refs, 2)
    all_up, all_down, h_all, a_all, g_all, du_all = take(refs, 6)
    wu, wd, rows_buf, u_buf, act, dpre, part, slots = take(refs, 8)
    held_up, held_down = take(refs, 2)
    up_part, up_sib, up_slots, down_part, down_sib, down_slots = take(refs, 6)
    a_in, g_in, h_in, du_in, g_last, t_buf = take(refs, 6)
    net = Net(*refs)
    top = layers - 1
    width, hidden = wu.shape[1], wu.shape[2]
    cols = hidden // NY
    piece = held_up.shape[2]
    tile = width // 8
    pieces_at = {dx: at(net.block(dx) * piece, piece) for dx in range(NX)}

    def start(copies):
        for copy in copies:
            copy.start()

    def wait(copies):
        for copy in copies:
            copy.wait()

    own_piece = pieces_at[0]

    def fetch_of(layer):
        return (PieceFetch(net, w_up.at[layer, own_piece], lambda slot: held_up.at[layer, slot]),
                PieceFetch(net, w_down.at[layer, :, own_piece], lambda slot: held_down.at[layer, slot * cols:(slot + 1) * cols]))

    def spread_of(layer):
        def up_view(dx, half):
            whole = all_up.at[layer, :, pieces_at[dx % NX]]
            return whole if half is None else whole.at[:, half * (piece // 2):(half + 1) * (piece // 2)]

        def down_view(dx, half):
            index, tall = net.block(dx), 3 * cols
            if half is None:
                return all_down.at[layer, index]
            return all_down.at[layer, index, half * (tall // 2):(half + 1) * (tall // 2)]

        return PieceSpread(net, held_up.at[layer], up_view), PieceSpread(net, held_down.at[layer], down_view)

    def up_loads(layer):
        b = layer % 2
        own = net.local(w_up.at[layer], wu.at[b, :, 0:cols])
        return own, [net.local(all_up.at[layer, s], wu.at[b, :, (s + 1) * cols:(s + 2) * cols]) for s in range(NY - 1)]

    def down_loads(layer):
        b = layer % 2
        own = net.local(w_down.at[layer], wd.at[b, 0:cols])
        return own, [net.local(all_down.at[layer, n], wd.at[b, cols:, n * piece:(n + 1) * piece]) for n in range(all_down.shape[1])]

    net.barrier()
    fetches = [fetch_of(0)]
    start(fetches[0])
    for ahead in range(1, layers - 1):
        fetches.append(fetch_of(ahead))
        start(fetches[ahead])
    loads = up_loads(0), down_loads(0)
    loads[0][0].start()
    loads[1][0].start()
    n_rows = rows_buf.shape[1]
    n_slice = n_rows // NZ
    first = [net.local(x_all.at[at(net.y * n_rows, n_rows)], rows_buf.at[0]),
             net.local(t_all.at[at(net.y * n_rows + net.z * n_slice, n_slice)], t_buf)]
    start(first)
    spread_up, spread_down = spread_of(0)
    fetches[0][0].arrived()
    spread_up.start()
    fetches[0][1].arrived()
    spread_down.start()
    spread_up.relay()
    spread_down.relay()
    spread_up.cross()
    spread_up.finish()
    start(loads[0][1])
    wait(first)
    per_part = 8 // PARTS

    h_rows, a_moves = {}, []
    for layer in range(layers):
        b = layer % 2
        h_ref, out_ref = rows_buf.at[b], rows_buf.at[1 - b]
        spreads, rows = None, None
        if layer > 0:
            rows = h_rows[layer] = RowGather(net, h_ref, h_all.at[layer - 1])
            rows.start()
            if layer < top:
                fetches[layer + 1][0].arrived()
                fetches[layer + 1][1].arrived()
                spreads = spread_of(layer + 1)
                start(spreads)
        loads[0][0].wait()
        wait(loads[0][1])

        @pl.loop(0, NY)
        def _(n):
            block = at(n * cols, cols)
            pre = jnp.dot(h_ref[...], wu[b, :, block], preferred_element_type=F32).astype(BF16)
            u_buf[layer, :, block] = pre
            act[:, block] = gelu_tanh(pre.astype(F32)).astype(BF16)

        exchange = ColumnExchange(net, act, a_all.at[layer])
        a_moves.append(exchange)
        if layer == 0:
            exchange.start()
            spread_down.cross()
            spread_down.finish()
            start(loads[1][1])
            fetches[1][0].arrived()
            fetches[1][1].arrived()
            spreads = spread_of(1)
            start(spreads)
        ring = z_ring(net, part, slots, out_ref)

        def down(n):
            part[:, at(n * tile, tile)] = jnp.dot(act[...], wd[b, :, at(n * tile, tile)], preferred_element_type=F32)

        loads[1][0].wait()
        wait(loads[1][1])
        for q in range(PARTS):
            pl.loop(q * per_part, (q + 1) * per_part)(down)
            ring.reduce_half(q)
        if layer == 0:
            fetches.append(fetch_of(top))
            start(fetches[top])
        else:
            exchange.start()
        for step in (1, 2, 3):
            ring.reduce_all(step)
        if spreads and layer > 0:
            spreads[0].relay()
            spreads[1].relay()
        for q in range(PARTS):
            value = ring.block(h_ref)(0, q)[...] + ring.total(q).astype(BF16)
            if layer == top:
                wide = value.shape[1]
                err = value.astype(F32) - t_buf[:, q * wide:(q + 1) * wide].astype(F32)
                value = (err / total_tokens).astype(BF16)
            ring.out(0, q)[...] = value
            ring.gather_half(q)
        if rows:
            rows.relay()
        if spreads and layer == 0:
            spreads[0].relay()
            spreads[1].relay()
        ring.gather_all(1)
        ring.gather_all(2)
        if spreads:
            spreads[0].cross()
            spreads[1].cross()
        ring.gather_all(3)
        if spreads:
            spreads[0].finish()
            spreads[1].finish()
            loads = up_loads(layer + 1), down_loads(layer + 1)
            for own, others in loads:
                own.start()
                start(others)
        if rows:
            rows.sent()
        exchange.sent()
        ring.arrived()
        ring.finish()
    for pair in fetches:
        pair[0].sent()
        pair[1].sent()

    def up_product(lo, hi):
        tall = up_part.shape[2]

        @pl.loop(lo, hi)
        def _(n):
            up_part[lax.div(n, 2), lax.rem(n, 2)] = lax.dot_general(
                h_in[:, at(n * tall, tall)], du_in[...], ROW_CONTRACT, preferred_element_type=F32)

    def down_product(lo, hi, g):
        @pl.loop(lo, hi)
        def _(n):
            block = at(n * tile, tile)
            value = lax.dot_general(a_in[...], g[:, block], ROW_CONTRACT, preferred_element_type=F32)
            down_part[:, :, :, block] = value.reshape(NX, 2, cols // 8, tile)

    def do(*actions):
        def job():
            for action in actions:
                action()
        return job

    def piece_of(ref, q, count=PARTS):
        wide = ref.shape[-1] // count
        return ref.at[(slice(None),) * (len(ref.shape) - 1) + (slice(q * wide, (q + 1) * wide),)]

    reload, prev_rows, prev_up, prev_down, prev_a, prev_layer = {}, None, None, None, None, None
    for layer in reversed(range(layers)):
        b = layer % 2
        g_ref, out_ref = rows_buf.at[1 - b], rows_buf.at[b]
        if layer > 0:
            h_rows[layer].finish()
        a_moves[layer].arrived()
        h_load = net.local(x_all if layer == 0 else h_all.at[layer - 1], h_in)
        h_load.start()
        a_load = net.local(a_all.at[layer], a_in)
        if layer == 0:
            pieces = [RowGather(net, piece_of(g_ref, q), piece_of(g_last, q)) for q in range(PARTS)]
            pieces[0].start()
        if layer in reload:
            reload[layer][0][0].wait()
            wait(reload[layer][0][1])

        @pl.loop(0, NY)
        def _(n):
            block = at(n * cols, cols)
            d_act = lax.dot_general(g_ref[...], wd[b, block, :], COL_CONTRACT, preferred_element_type=F32)
            _, gelu_vjp = jax.vjp(gelu_tanh, u_buf[layer, :, block].astype(F32))
            dpre[:, block] = gelu_vjp(d_act)[0].astype(BF16)

        exchange = ColumnExchange(net, dpre, du_all.at[layer])
        exchange.start()
        du_load = net.local(du_all.at[layer], du_in)
        if layer == 0:
            break
        rows = [RowGather(net, piece_of(g_ref, k, 2), piece_of(g_all.at[layer], k, 2)) for k in (0, 1)]
        for gather in rows:
            gather.start()
        if layer in reload:
            reload[layer][1][0].wait()
            wait(reload[layer][1][1])
        ring = z_ring(net, part, slots, out_ref)

        def back(n):
            part[:, at(n * tile, tile)] = lax.dot_general(
                dpre[...], wu[b, at(n * tile, tile), :], COL_CONTRACT, preferred_element_type=F32)

        for q in range(PARTS):
            pl.loop(q * per_part, (q + 1) * per_part)(back)
            ring.reduce_half(q)
        if layer >= 2:
            reload[layer - 2] = (down_loads(layer - 2), up_loads(layer - 2)) if layer > 2 else (down_loads(0),)
            for own, others in reload[layer - 2]:
                own.start()
                start(others)
        jobs = {name: [] for name in ("r1", "r2", "r3", "t", "g1", "g2", "g3")}
        up_sum = GradSum(net, up_part, up_sib, up_slots, grad_up.at[layer])
        down_sum = None
        if prev_down:
            jobs["r1"] += [prev_down.relay]
        if prev_rows:
            down_sum = GradSum(net, down_part, down_sib, down_slots, grad_down.at[prev_layer])
            g_load = net.local(g_all.at[prev_layer], g_in)
            jobs["r1"] += [prev_up.settle, do(prev_rows[0].finish, prev_rows[1].finish, g_load.start)]
            if prev_down:
                jobs["r2"] += [do(prev_down.finish, prev_down.end)]
            jobs["r2"] += [do(g_load.wait, prev_a.wait, functools.partial(down_product, 0, 2, g_in))]
            jobs["r2"] += [functools.partial(down_product, n, n + 2, g_in) for n in (2, 4)]
            jobs["r2"] += [do(functools.partial(down_product, 6, 8, g_in), down_sum.swap.start, a_load.start), prev_up.relay]
        else:
            jobs["r2"] += [a_load.start]
        jobs["r3"] += [do(exchange.sent, exchange.arrived, du_load.start)]
        if prev_rows:
            jobs["r3"] += [down_sum.merge, prev_up.finish]
            jobs["t"] += [prev_up.end]
        jobs["t"] += [do(h_load.wait, du_load.wait, functools.partial(up_product, 0, 2))]
        jobs["t"] += [functools.partial(up_product, n, n + 2) for n in (2, 4)]
        jobs["t"] += [do(functools.partial(up_product, 6, 8), up_sum.swap.start), rows[0].relay]
        jobs["g1"] += [up_sum.merge]
        if down_sum:
            jobs["g1"] += [down_sum.step]
            jobs["g3"] += [down_sum.settle]
        jobs["g3"] += [up_sum.step]
        ring.reduce_all(1, jobs["r1"])
        ring.reduce_all(2, jobs["r2"])
        ring.reduce_all(3, jobs["r3"])
        for q in range(PARTS):
            total = ring.total(q)
            ring.out(0, q)[...] = (ring.block(g_ref)(0, q)[...].astype(F32) + total).astype(BF16)
            ring.gather_half(q)
            if q + 1 < PARTS:
                jobs["t"].pop(0)()
        for job in jobs["t"]:
            job()
        ring.gather_all(1, jobs["g1"])
        ring.gather_all(2, jobs["g2"])
        ring.gather_all(3, jobs["g3"])
        rows[1].relay()
        for gather in rows:
            gather.sent()
        ring.arrived()
        ring.finish()
        prev_rows, prev_up, prev_down, prev_a, prev_layer = rows, up_sum, down_sum, a_load, layer

    pieces[1].start()
    if prev_down:
        prev_down.relay()
    prev_up.settle()
    for gather in prev_rows:
        gather.finish()
    g_load = net.local(g_all.at[prev_layer], g_in)
    g_load.start()
    if prev_down:
        prev_down.finish()
        prev_down.end()
    g_load.wait()
    prev_a.wait()
    down_sum = GradSum(net, down_part, down_sib, down_slots, grad_down.at[prev_layer])
    down_product(0, 8, g_in)
    down_sum.swap.start()
    a_load.start()
    prev_up.relay()
    exchange.sent()
    exchange.arrived()
    du_load.start()
    down_sum.merge()
    pieces[0].relay()
    pieces[2].start()
    prev_up.finish()
    prev_up.end()
    h_load.wait()
    du_load.wait()
    up_sum = GradSum(net, up_part, up_sib, up_slots, grad_up.at[0])
    up_product(0, 8)
    up_sum.swap.start()
    down_sum.step()
    pieces[1].relay()
    pieces[3].start()
    up_sum.merge()
    down_sum.settle()
    pieces[2].relay()
    up_sum.step()
    down_sum.relay()
    pieces[3].relay()
    up_sum.settle()
    down_sum.finish()
    down_sum.end()
    a_load.wait()
    sums = []
    for q in range(PARTS):
        pieces[q].sent()
        pieces[q].finish()
        down_product(q * per_part, (q + 1) * per_part, g_last)
        sums.append(GradSum(net, piece_of(down_part, q), piece_of(down_sib, q), piece_of(down_slots, q), piece_of(grad_down.at[0], q)))
        sums[q].swap.start()
        if q == 1:
            up_sum.relay()
        if q == 2:
            sums[0].step()
        sums[q].merge()
    up_sum.finish()
    sums[1].step()
    sums[0].settle()
    sums[2].step()
    sums[1].settle()
    sums[3].step()
    sums[2].settle()
    sums[0].relay()
    sums[3].settle()
    for q in (1, 2, 3):
        sums[q].relay()
    up_sum.end()
    for q in range(PARTS):
        sums[q].finish()
    for q in range(PARTS):
        sums[q].end()


def local_step(hidden, targets, w_up, w_down, n_dp):
    layers, width, cols = w_up.shape
    tokens = hidden.shape[0]
    rows, inner, piece = tokens // NY, cols * NY, width // n_dp
    up_shape, down_shape = (NX, 2, width // 8, cols), (NX, 2, cols // 8, width)

    def out(dtype, *shape):
        return jax.ShapeDtypeStruct(shape, dtype)

    outs = [out(F32, layers, *up_shape), out(F32, layers, *down_shape),
            out(BF16, layers, NY - 1, width, cols), out(BF16, layers, n_dp, (NY - 1) * cols, piece),
            out(BF16, layers - 1, tokens, width), out(BF16, layers, tokens, cols),
            out(BF16, layers, tokens, width), out(BF16, layers, tokens, cols)]

    def sum_scratch(shape):
        return [pltpu.VMEM(shape, F32), pltpu.VMEM((NX, *shape[2:]), F32), pltpu.VMEM((6, shape[2] // 2, shape[3]), F32)]

    scratch = [pltpu.VMEM((2, width, inner), BF16), pltpu.VMEM((2, inner, width), BF16), pltpu.VMEM((2, rows, width), BF16),
               pltpu.VMEM((layers, rows, inner), BF16), pltpu.VMEM((rows, inner), BF16), pltpu.VMEM((rows, inner), BF16),
               pltpu.VMEM((rows, width), F32), pltpu.VMEM((7 * PARTS, rows // NZ, width // PARTS), F32),
               pltpu.VMEM((layers, NY - 1, piece, cols), BF16), pltpu.VMEM((layers, (NY - 1) * cols, piece), BF16),
               *sum_scratch(up_shape), *sum_scratch(down_shape),
               pltpu.VMEM((tokens, cols), BF16), pltpu.VMEM((tokens, width), BF16), pltpu.VMEM((tokens, width), BF16), pltpu.VMEM((tokens, cols), BF16),
               pltpu.VMEM((tokens, width), BF16), pltpu.VMEM((rows // NZ, width), BF16),
               pltpu.SemaphoreType.DMA((COPIES,)), pltpu.SemaphoreType.DMA((COPIES,)), pltpu.SemaphoreType.DMA((LOCALS,))]
    up, down = pl.pallas_call(
        functools.partial(step_kernel, layers, tokens * n_dp), out_shape=outs, in_specs=[ANY] * 4,
        out_specs=[ANY] * len(outs), scratch_shapes=scratch, name="step",
        compiler_params=pltpu.CompilerParams(collective_id=0, has_side_effects=True, vmem_limit_bytes=60 * 1024 * 1024),
    )(hidden, targets, w_up, w_down)[:2]
    return up.reshape(layers, width, cols), down.reshape(layers, cols, width)


def solution(mesh):
    n_dp = mesh.shape["dp"]

    def grad_step(hidden_in, targets, w_up, w_down):
        step_fn = functools.partial(local_step, n_dp=n_dp)
        mapped = jax.shard_map(step_fn, mesh=mesh, in_specs=(P("dp", None), P("dp", None), P(None, None, "tp"), P(None, "tp", None)), out_specs=(P(None, None, "tp"), P(None, "tp", None)), check_vma=False)
        return mapped(hidden_in, targets, w_up, w_down)

    return grad_step
```
